32 devices in a mesh: mesh: 8 (over z, y), pts: 4 (over x, core).
Axes of the slice: x: 2, y: 2, z: 4, core: 2. Of those that a mesh axis runs over, the one named last changes fastest.
Arguments:
- inputs: float32 [32768, 8], P(('mesh', 'pts')), may hold values from -6 to 6
- target: float32 [32768, 4], P(('mesh', 'pts')), may hold values from -6 to 6
- lengths: int32 [8, 4], P('mesh'), may hold values from 1 to 2048, 4096 in all within a row
- step_count: int32 [1], replicated, may hold values from 2 to 20
- muon_weight: float32 [2, 5, 256, 256], P(None, None, ('mesh', 'pts')), may hold values from -0.375 to 0.375
- muon_moment: float32 [2, 5, 256, 256], P(None, None, ('mesh', 'pts')), may hold values from -0.0017089844 to 0.0017089844
- adam_weight: float32 [18848], P(('mesh', 'pts'))
- adam_first: float32 [18848], P(('mesh', 'pts')), may hold values from -0.0004272461 to 0.0004272461
- adam_second: float32 [18848], P(('mesh', 'pts')), may hold values from 2e-11 to 4e-09
Outputs:
- new_muon_weight: float32 [2, 5, 256, 256], P(None, None, ('mesh', 'pts'))
- new_muon_moment: float32 [2, 5, 256, 256], P(None, None, ('mesh', 'pts'))
- new_adam_weight: float32 [18848], P(('mesh', 'pts'))
- new_adam_first: float32 [18848], P(('mesh', 'pts'))
- new_adam_second: float32 [18848], P(('mesh', 'pts'))
- step_loss: float32 [], replicated
- clip_norm: float32 [], replicated
The draws below stay inside these ranges and needn't reach their ends.
Inputs may be any that keep to these rules, and one draw needn't show every extreme that they name: Each group's 4 lengths sum to 4096, and the largest of each group is exactly half of that.
All inputs are finite; a program needn't handle non-finite values.
Results may differ from the reference program's by a relative error of at most 0.0003.
Values sent between devices are 32-bit elements; how exact they have to be, the bound alone decides.
A program may use at most 192 MiB of HBM per device.

```python
import math
import jax
import jax.numpy as jnp
import numpy as np
from jax import lax

C = 256
H = 8
DH = 32
S = 64
IN = 8
OUT = 4
L = 2
MPG = 4
ROWS_DEV = 1024
NPOINTS = 32768
RAW = 18836
FLAT = 18848
N_MESH = 8
N_PTS = 4


def draw_adam_weight(key, part):
    offsets = np.zeros(FLAT, np.float32)
    widths = np.full(FLAT, 0.1, np.float32)
    pieces = [('emb_w', IN * C, 0.0, IN ** (-0.5)), ('emb_b', C, 0.0, 0.3), ('head_w', C * OUT, 0.0, C ** (-0.5)), ('head_b', OUT, 0.0, 0.3), ('fin_gain', C, 1.0, 0.2), ('fin_bias', C, 0.0, 0.2), ('qkv', L * 3 * DH * DH, 0.0, DH ** (-0.5)), ('slice_w', L * DH * S, 0.0, 2.0 * DH ** (-0.5)), ('slice_b', L * S, 0.0, 0.5), ('temp', L * H, 1.0, 0.25)]
    offset = 0
    for label_text, extent, centre, width in pieces:
        offsets[offset:offset + extent] = centre
        widths[offset:offset + extent] = width
        offset = offset + extent
    for layer_index in range(L):
        for row_index in range(9):
            centre = 1.0 if row_index in (0, 5) else 0.0
            offsets[offset:offset + C] = centre
            widths[offset:offset + C] = 0.2
            offset = offset + C
    noise = jax.random.uniform(key, (FLAT,), jnp.float32, -math.sqrt(3.0), math.sqrt(3.0))
    return jnp.asarray(offsets) + jnp.asarray(widths) * noise


def draw_target(key, part):
    values = jax.random.normal(jax.random.fold_in(key, 13), (NPOINTS, OUT), jnp.float32)
    return jnp.clip(values, -6.0, 6.0)


def levels(rng, shape, split, low, largest):
    loudness = 1.0
    for axis_at, shards_of in split:
        draws = jax.random.uniform(jax.random.fold_in(jax.random.fold_in(rng, 6), axis_at), (shards_of,), jnp.float32, low / len(split), largest / len(split))
        loudness = loudness * jnp.repeat(jnp.exp(draws), shape[axis_at] // shards_of).reshape((-1,) + (1,) * (len(shape) - 1 - axis_at))
    return loudness


def split_up(amount, total, most, lean):
    weights = [(1 << 20) // math.isqrt(rank ** lean) + 1 for rank in range(2, amount + 1)]
    surplus, given = total - most - (amount - 1), [1] * (amount - 1)
    while surplus > 0:
        candidates = [i for i in range(amount - 1) if given[i] < most]
        whole, budget = sum([weights[i] for i in candidates]), surplus
        for i in candidates:
            more = min(most - given[i], max(1, budget * weights[i] // whole), surplus)
            given[i] = given[i] + more
            surplus = surplus - more
    return np.array([most] + given)


def uneven_parts(own_key, number_of, total, bound, lean):
    if number_of == 2:
        one = jax.random.randint(own_key, (), max(1, total - bound), min(bound, total - 1) + 1)
        return jnp.stack([one, total - one])
    sizes = jnp.asarray(split_up(number_of, total, bound, lean), jnp.int32)
    couples = (number_of - 1) // 2
    donor, taker = sizes[1:1 + 2 * couples:2], sizes[2:2 + 2 * couples:2]
    room = jnp.minimum(donor - 1, bound - taker)
    shifted = jax.random.randint(jax.random.fold_in(own_key, 1), (couples,), 0, 1 << 20) % (room + 1)
    sizes = sizes.at[1:1 + 2 * couples:2].set(donor - shifted).at[2:2 + 2 * couples:2].set(taker + shifted)
    return sizes[jax.random.permutation(jax.random.fold_in(own_key, 2), number_of)]


def normal_values(rng, shape, scale, most, cuts=(), kind=jnp.bfloat16):
    level = levels(rng, shape, cuts, -0.22, 0.18) if cuts else 1.0
    entries = jax.random.normal(rng, shape, jnp.float32) * scale * level
    return jnp.minimum(jnp.maximum(entries, -most), most).astype(kind)


def setup_inputs(seed: int = 0) -> dict:
    keys = jax.random.split(jax.random.key(seed), 10)
    inputs = normal_values(keys[0], (NPOINTS, IN), 1.0, 6.0, ((0, 32),), jnp.float32)
    target = draw_target(jax.random.fold_in(keys[9], 71), 0)
    lengths = jax.vmap(lambda own: uneven_parts(own, MPG, ROWS_DEV * N_PTS, ROWS_DEV * N_PTS // 2, 2))(jax.random.split(keys[2], N_MESH)).reshape((N_MESH, MPG)).astype(jnp.int32)
    step_count = jax.random.randint(keys[3], (1,), 2, 21).astype(jnp.int32)
    muon_weight = normal_values(keys[4], (L, 5, C, C), C ** -0.5, 0.375, ((2, 32),), jnp.float32)
    muon_moment = normal_values(keys[5], (L, 5, C, C), (0.1 / (L * 5 * C * C + RAW) ** 0.5), 0.0017089844, ((2, 32),), jnp.float32)
    adam_weight = draw_adam_weight(jax.random.fold_in(keys[9], 71), 0)
    adam_first = normal_values(keys[7], (FLAT,), 0.00003, 0.0004272461, ((0, 32),), jnp.float32)
    adam_second = jnp.clip(jnp.exp(math.log(3.999999886872274e-09) - 5.2983173 * jax.random.uniform(keys[8], (FLAT,), jnp.float32) ** levels(keys[8], (FLAT,), ((0, 32),), -0.2, 0.2)), 1.9999999920083944e-11, 3.999999886872274e-09)
    return dict(inputs=inputs, target=target, lengths=lengths, step_count=step_count, muon_weight=muon_weight, muon_moment=muon_moment, adam_weight=adam_weight, adam_first=adam_first, adam_second=adam_second)


HIGH = lax.Precision.HIGHEST
ns_a = 3.4445
ns_b = -4.775
ns_c = 2.0315
peak_rate = 0.3
warm_steps = 12.0
total_steps = 40.0

@jax.custom_vjp
def low(v):
    return lax.optimization_barrier(v.astype(jnp.bfloat16)).astype(jnp.float32)

@jax.custom_vjp
def low_back(v):
    return v

def low_keep(v):
    return (low(v), None)

def low_pass(kept, grad):
    return (grad,)

def back_keep(v):
    return (v, None)

def back_low(kept, grad):
    return (low(grad),)
low.defvjp(low_keep, low_pass)
low_back.defvjp(back_keep, back_low)

def layout():
    pieces = [('emb_w', (IN, C)), ('emb_b', (C,)), ('head_w', (C, OUT)), ('head_b', (OUT,)), ('fin', (2, C)), ('qkv', (L, 3, DH, DH)), ('slice_w', (L, DH, S)), ('slice_b', (L, S)), ('temp', (L, H)), ('vec', (L, 9, C))]
    places = {}
    offset = 0
    for label_text, extent in pieces:
        places[label_text] = (offset, extent)
        offset = offset + math.prod(extent)
    return places

def unpack(packed):
    return {label_text: packed[offset:offset + math.prod(extent)].reshape(extent) for label_text, (offset, extent) in layout().items()}

def matmul(left, right):
    return jnp.dot(left, right, precision=HIGH)

def norm_rows(values, gain, shift):
    centre = values - lax.optimization_barrier(jnp.mean(values, axis=-1, keepdims=True))
    spread = lax.optimization_barrier(jnp.mean(centre * centre, axis=-1, keepdims=True))
    return centre * lax.rsqrt(spread + 1e-05) * gain + shift

def mesh_mask(lengths_row, first, points):
    ends = jnp.cumsum(lengths_row)
    starts = ends - lengths_row
    position = first + jnp.arange(points, dtype=jnp.int32)
    inside = (position[:, None] >= starts[None, :]) & (position[:, None] < ends[None, :])
    return inside.astype(jnp.float32)

def embed_piece(inputs, packed):
    params = unpack(packed)
    return matmul(inputs, params['emb_w']) + params['emb_b']

def slice_piece(hidden, matrices, packed, layer_index, onehot):
    params = unpack(packed)
    vectors = params['vec'][layer_index]
    points = hidden.shape[0]
    normed = norm_rows(hidden, vectors[0], vectors[1])
    features = (matmul(normed, matrices[0]) + vectors[2]).reshape(points, H, DH)
    routed = (matmul(normed, matrices[1]) + vectors[3]).reshape(points, H, DH)
    logits = jnp.einsum('phd,ds->phs', routed, params['slice_w'][layer_index], precision=HIGH)
    logits = (logits + params['slice_b'][layer_index]) / params['temp'][layer_index][:, None]
    weights = jax.nn.softmax(logits, axis=-1)
    numerator = jnp.einsum('pm,phs,phd->mhsd', onehot, weights, features, precision=HIGH)
    denominator = jnp.einsum('pm,phs->mhs', onehot, weights, precision=HIGH)
    return (weights, numerator, denominator)

def mix_piece(numerator, denominator, packed, layer_index):
    triple = unpack(packed)['qkv'][layer_index]
    tokens = numerator / (denominator[..., None] + 1e-05)
    queries = jnp.einsum('mhsd,de->mhse', tokens, triple[0], precision=HIGH)
    keys_all = jnp.einsum('mhsd,de->mhse', tokens, triple[1], precision=HIGH)
    values = jnp.einsum('mhsd,de->mhse', tokens, triple[2], precision=HIGH)
    scores = jnp.einsum('mhsd,mhtd->mhst', queries, keys_all, precision=HIGH) * DH ** (-0.5)
    return jnp.einsum('mhst,mhtd->mhsd', jax.nn.softmax(scores, axis=-1), values, precision=HIGH)

def out_piece(hidden, weights, mixed, matrices, packed, layer_index, onehot):
    vectors = unpack(packed)['vec'][layer_index]
    points = hidden.shape[0]
    spread_wts = onehot[:, :, None, None] * weights[:, None, :, :]
    pointwise = jnp.einsum('pmhs,mhsd->phd', spread_wts, mixed, precision=HIGH).reshape(points, C)
    hidden = hidden + matmul(pointwise, matrices[2]) + vectors[4]
    normed = norm_rows(hidden, vectors[5], vectors[6])
    inner = jax.nn.gelu(matmul(normed, matrices[3]) + vectors[7], approximate=False)
    return hidden + matmul(inner, matrices[4]) + vectors[8]

def head_piece(hidden, packed, target, onehot):
    params = unpack(packed)
    normed = norm_rows(hidden, params['fin'][0], params['fin'][1])
    predicted = matmul(normed, params['head_w']) + params['head_b']
    misfit = predicted - target
    errors = matmul(onehot.T, lax.optimization_barrier(jnp.sum(misfit * misfit, axis=-1)))
    scales = matmul(onehot.T, lax.optimization_barrier(jnp.sum(target * target, axis=-1)))
    return (errors, scales)

def loss_piece(errors, scales, meshes, floor_value):
    return jnp.sum(jnp.sqrt((errors + 1e-06) / jnp.maximum(scales, floor_value))) / meshes

def one_cycle(count):
    start_rate = peak_rate / 25.0
    end_rate = start_rate / 10000.0
    rising = start_rate + (peak_rate - start_rate) * 0.5 * (1.0 - jnp.cos(math.pi * count / warm_steps))
    falling = end_rate + (peak_rate - end_rate) * 0.5 * (1.0 + jnp.cos(math.pi * (count - warm_steps) / (total_steps - warm_steps)))
    return jnp.where(count <= warm_steps, rising, falling)

def newton_schulz(current, gram_of):
    for sweep in range(5):
        gram = gram_of(current)
        product = jnp.einsum('...rc,...cd->...rd', current, gram, precision=HIGH)
        current = ns_a * current + ns_b * product + ns_c * jnp.einsum('...rc,...cd->...rd', product, gram, precision=HIGH)
    return current

def apply_update(grad_muon, grad_adam, square_sum, step_count, muon_weight, muon_moment, adam_weight, adam_first, adam_second, frob_of, orthogonal_of):
    norm_value = jnp.sqrt(square_sum)
    factor = 0.1 / jnp.maximum(norm_value, 0.1)
    moment = 0.95 * muon_moment + factor * grad_muon
    normalized = moment / (jnp.sqrt(frob_of(moment)) + 1e-07)[..., None, None]
    current = orthogonal_of(normalized)
    count = step_count[0].astype(jnp.float32)
    rate = one_cycle(count)
    new_muon = muon_weight * (1.0 - rate * 0.01) - rate * (0.2 * C ** 0.5) * current
    clipped = factor * grad_adam
    first = 0.9 * adam_first + 0.1 * clipped
    second = 0.999 * adam_second + 0.001 * clipped * clipped
    first_hat = first / (1.0 - 0.9 ** count)
    second_hat = second / (1.0 - 0.999 ** count)
    new_adam = adam_weight * (1.0 - rate * 0.01) - rate * first_hat / (jnp.sqrt(second_hat) + 1e-08)
    return (new_muon, moment, new_adam, first, second, norm_value)

def reference(inputs, target, lengths, step_count, muon_weight, muon_moment, adam_weight, adam_first, adam_second):
    group_rows = ROWS_DEV * N_PTS
    floor_value = float(ROWS_DEV * N_PTS)
    inputs_grouped = inputs.reshape(N_MESH, group_rows, IN)
    target_grouped = target.reshape(N_MESH, group_rows, OUT)

    def one_group(carried, sliced):
        part_inputs, part_target, part_lengths = sliced
        onehot = mesh_mask(part_lengths, 0, group_rows)

        def loss_of(matrices_all, packed):
            hidden = embed_piece(part_inputs, packed)
            for layer_index in range(L):
                weights, numerator, denominator = slice_piece(hidden, matrices_all[layer_index], packed, layer_index, onehot)
                mixed = mix_piece(numerator, denominator, packed, layer_index)
                hidden = out_piece(hidden, weights, mixed, matrices_all[layer_index], packed, layer_index, onehot)
            errors, scales = head_piece(hidden, packed, part_target, onehot)
            return loss_piece(errors, scales, N_MESH * MPG, floor_value)
        loss_value, backward = jax.vjp(loss_of, muon_weight, adam_weight)
        grad_muon, grad_adam = backward(jnp.ones_like(loss_value))
        return ((carried[0] + loss_value, carried[1] + grad_muon, carried[2] + grad_adam), None)
    initial = (jnp.zeros((), jnp.float32), jnp.zeros_like(muon_weight), jnp.zeros_like(adam_weight))
    (loss_total, grad_muon, grad_adam), unused_rest = lax.scan(one_group, initial, (inputs_grouped, target_grouped, lengths))
    square_sum = jnp.sum(grad_muon * grad_muon) + jnp.sum(grad_adam * grad_adam)

    def frob_of(moment):
        return lax.optimization_barrier(jnp.sum(moment * moment, axis=(2, 3)))

    def gram_of(current):
        return jnp.einsum('...rc,...rd->...cd', current, current, precision=HIGH)

    def orthogonal_of(normalized):
        return newton_schulz(normalized, gram_of)
    results = apply_update(grad_muon, grad_adam, square_sum, step_count, muon_weight, muon_moment, adam_weight, adam_first, adam_second, frob_of, orthogonal_of)
    return (results[0], results[1], results[2], results[3], results[4], loss_total, results[5])
```

```python
from functools import partial
import math

import jax
import jax.numpy as jnp
from jax import lax
from jax.experimental import pallas as pl
from jax.experimental.pallas import tpu as pltpu
from jax.sharding import PartitionSpec as P

C = 256
H = 8
DH = 32
S = 64
IN = 8
OUT = 4
L = 2


HIGH = lax.Precision.HIGH
ns_a = 3.4445
ns_b = -4.775
ns_c = 2.0315
peak_rate = 0.3
warm_steps = 12.0
total_steps = 40.0


def layout():
    pieces = [
        ("emb_w", (IN, C)),
        ("emb_b", (C,)),
        ("head_w", (C, OUT)),
        ("head_b", (OUT,)),
        ("fin", (2, C)),
        ("qkv", (L, 3, DH, DH)),
        ("slice_w", (L, DH, S)),
        ("slice_b", (L, S)),
        ("temp", (L, H)),
        ("vec", (L, 9, C)),
    ]
    places = {}
    offset = 0
    for label_text, extent in pieces:
        places[label_text] = (offset, extent)
        offset = offset + math.prod(extent)
    return places


def unpack(packed):
    return {
        label_text: packed[offset : offset + math.prod(extent)].reshape(extent)
        for label_text, (offset, extent) in layout().items()
    }


def matmul(left, right):
    return jnp.dot(left, right, precision=HIGH)


def norm_rows(values, gain, shift):
    centre = values - jnp.mean(values, axis=-1, keepdims=True)
    spread = jnp.mean(centre * centre, axis=-1, keepdims=True)
    return centre * lax.rsqrt(spread + 1e-05) * gain + shift


def mesh_mask(lengths_row, first, points):
    ends = jnp.cumsum(lengths_row)
    starts = ends - lengths_row
    position = first + jnp.arange(points, dtype=jnp.int32)
    inside = (position[:, None] >= starts[None, :]) & (position[:, None] < ends[None, :])
    return inside.astype(jnp.float32)


def embed_piece(inputs, packed):
    params = unpack(packed)
    return matmul(inputs, params["emb_w"]) + params["emb_b"]


def slice_piece(hidden, matrices, packed, layer_index, onehot):
    params = unpack(packed)
    vectors = params["vec"][layer_index]
    points = hidden.shape[0]
    normed = norm_rows(hidden, vectors[0], vectors[1])
    features = (matmul(normed, matrices[0]) + vectors[2]).reshape(points, H, DH)
    routed = (matmul(normed, matrices[1]) + vectors[3]).reshape(points, H, DH)
    logits = jnp.einsum("phd,ds->phs", routed, params["slice_w"][layer_index], precision=HIGH)
    logits = (logits + params["slice_b"][layer_index]) / params["temp"][layer_index][:, None]
    weights = jax.nn.softmax(logits, axis=-1)
    numerator = jnp.einsum("pm,phs,phd->mhsd", onehot, weights, features, precision=HIGH)
    denominator = jnp.einsum("pm,phs->mhs", onehot, weights, precision=HIGH)
    return (weights, numerator, denominator)


def mix_piece(numerator, denominator, packed, layer_index):
    triple = unpack(packed)["qkv"][layer_index]
    tokens = numerator / (denominator[..., None] + 1e-05)
    queries = jnp.einsum("mhsd,de->mhse", tokens, triple[0], precision=HIGH)
    keys_all = jnp.einsum("mhsd,de->mhse", tokens, triple[1], precision=HIGH)
    values = jnp.einsum("mhsd,de->mhse", tokens, triple[2], precision=HIGH)
    scores = jnp.einsum("mhsd,mhtd->mhst", queries, keys_all, precision=HIGH) * DH ** (-0.5)
    return jnp.einsum("mhst,mhtd->mhsd", jax.nn.softmax(scores, axis=-1), values, precision=HIGH)


def out_piece(hidden, weights, mixed, matrices, packed, layer_index, onehot):
    vectors = unpack(packed)["vec"][layer_index]
    points = hidden.shape[0]
    spread_wts = onehot[:, :, None, None] * weights[:, None, :, :]
    pointwise = jnp.einsum("pmhs,mhsd->phd", spread_wts, mixed, precision=HIGH).reshape(points, C)
    hidden = hidden + matmul(pointwise, matrices[2]) + vectors[4]
    normed = norm_rows(hidden, vectors[5], vectors[6])
    inner = jax.nn.gelu(matmul(normed, matrices[3]) + vectors[7], approximate=False)
    return hidden + matmul(inner, matrices[4]) + vectors[8]


def head_piece(hidden, packed, target, onehot):
    params = unpack(packed)
    normed = norm_rows(hidden, params["fin"][0], params["fin"][1])
    predicted = matmul(normed, params["head_w"]) + params["head_b"]
    misfit = predicted - target
    errors = matmul(onehot.T, jnp.sum(misfit * misfit, axis=-1))
    scales = matmul(onehot.T, jnp.sum(target * target, axis=-1))
    return (errors, scales)


def loss_piece(errors, scales, meshes, floor_value):
    return jnp.sum(jnp.sqrt((errors + 1e-06) / jnp.maximum(scales, floor_value))) / meshes


def one_cycle(count):
    start_rate = peak_rate / 25.0
    end_rate = start_rate / 10000.0
    rising = start_rate + (peak_rate - start_rate) * 0.5 * (
        1.0 - jnp.cos(math.pi * count / warm_steps)
    )
    falling = end_rate + (peak_rate - end_rate) * 0.5 * (
        1.0 + jnp.cos(math.pi * (count - warm_steps) / (total_steps - warm_steps))
    )
    return jnp.where(count <= warm_steps, rising, falling)


def newton_schulz(current, gram_of):
    for sweep in range(5):
        gram = gram_of(current)
        product = jnp.einsum("...rc,...cd->...rd", current, gram, precision=HIGH)
        current = (
            ns_a * current
            + ns_b * product
            + ns_c * jnp.einsum("...rc,...cd->...rd", product, gram, precision=HIGH)
        )
    return current


def apply_update(
    grad_muon,
    grad_adam,
    square_sum,
    step_count,
    muon_weight,
    muon_moment,
    adam_weight,
    adam_first,
    adam_second,
    frob_of,
    orthogonal_of,
):
    norm_value = jnp.sqrt(square_sum)
    factor = 0.1 / jnp.maximum(norm_value, 0.1)
    moment = 0.95 * muon_moment + factor * grad_muon
    normalized = moment / (jnp.sqrt(frob_of(moment)) + 1e-07)[..., None, None]
    current = orthogonal_of(normalized)
    count = step_count[0].astype(jnp.float32)
    rate = one_cycle(count)
    new_muon = muon_weight * (1.0 - rate * 0.01) - rate * (0.2 * C**0.5) * current
    clipped = factor * grad_adam
    first = 0.9 * adam_first + 0.1 * clipped
    second = 0.999 * adam_second + 0.001 * clipped * clipped
    first_hat = first / (1.0 - 0.9**count)
    second_hat = second / (1.0 - 0.999**count)
    new_adam = adam_weight * (1.0 - rate * 0.01) - rate * first_hat / (jnp.sqrt(second_hat) + 1e-08)
    return (new_muon, moment, new_adam, first, second, norm_value)


MESH = pl.DeviceIdType.MESH
SLAB = (8, 256)


def grid_of(mesh_count, pts_count):
    cores = 2 if pts_count % 2 == 0 else 1
    rows = max(math.isqrt(mesh_count // 2), 1)
    while mesh_count % rows:
        rows -= 1
    return mesh_count // rows, rows, pts_count // cores, cores


def place_of(dims):
    planes, rows, columns, cores = dims
    across, along = lax.axis_index("mesh"), lax.axis_index("pts")
    return across // rows, across % rows, along // cores, along % cores


def device_at(dims, spot):
    z, y, x, c = spot
    return {"mesh": z * dims[1] + y, "pts": x * dims[3] + c}


def line_partners(dims, spot):
    found = []
    for axis in range(4):
        for step in range(1, dims[axis]):
            other = list(spot)
            other[axis] = lax.rem(spot[axis] + step, dims[axis])
            found.append(device_at(dims, other))
    return found


def greet(partners):
    barrier = pltpu.get_barrier_semaphore()
    for partner in partners:
        pl.semaphore_signal(barrier, inc=1, device_id=partner, device_id_type=MESH)
    pl.semaphore_wait(barrier, len(partners))


class Mail:
    def __init__(self, send_sems, recv_sems):
        self.send_sems, self.recv_sems, self.used, self.open = send_sems, recv_sems, 0, []

    def send(self, source, target, device):
        copy = pltpu.make_async_remote_copy(
            src_ref=source,
            dst_ref=target,
            send_sem=self.send_sems.at[self.used],
            recv_sem=self.recv_sems.at[self.used],
            device_id=device,
            device_id_type=MESH,
        )
        copy.start()
        self.used += 1
        self.open.append(copy)
        return copy

    def close(self):
        for copy in self.open:
            copy.wait_send()


def gather_kernel(dims, a_in, b_in, c_in, a_all, b_all, c_all, keep, send_sems, recv_sems):
    planes, rows, columns, cores = dims
    z, y, x, c = spot = place_of(dims)
    own = []
    for index, (source, target) in enumerate(
        ((a_in, a_all.at[c, x, y, z]), (b_in, b_all.at[c, y, x, z]), (c_in, c_all.at[c, x, y, z]))
    ):
        copy = pltpu.make_async_copy(source, target, keep.at[index])
        copy.start()
        own.append(copy)
    greet(line_partners(dims, spot))
    mail = Mail(send_sems, recv_sems)
    waits = []
    for step in range(1, planes):
        device = device_at(dims, (lax.rem(z + step, planes), y, x, c))
        waits.append(mail.send(a_in, a_all.at[c, x, y, z], device))
        waits.append(mail.send(b_in, b_all.at[c, y, x, z], device))
        waits.append(mail.send(c_in, c_all.at[c, x, y, z], device))
    for copy in own:
        copy.wait()
    for copy in waits:
        copy.wait_recv()
    partner = [device_at(dims, (z, y, x, lax.rem(c + step, cores))) for step in range(1, cores)]
    last = []

    def share(reference):
        for device in partner:
            last.append(mail.send(reference, reference, device))

    waits = []
    for step in range(1, rows):
        device = device_at(dims, (z, lax.rem(y + step, rows), x, c))
        for full in (a_all, c_all):
            waits.append(mail.send(full.at[c, x, y], full.at[c, x, y], device))
    for step in range(1, columns):
        device = device_at(dims, (z, y, lax.rem(x + step, columns), c))
        waits.append(mail.send(b_all.at[c, y, x], b_all.at[c, y, x], device))
    for reference in (a_all.at[c, x, y], b_all.at[c, y, x], c_all.at[c, x, y]):
        share(reference)
    for copy in waits:
        copy.wait_recv()
    waits = []
    for step in range(1, columns):
        device = device_at(dims, (z, y, lax.rem(x + step, columns), c))
        for full in (a_all, c_all):
            waits.append(mail.send(full.at[c, x], full.at[c, x], device))
    for step in range(1, rows):
        device = device_at(dims, (z, lax.rem(y + step, rows), x, c))
        waits.append(mail.send(b_all.at[c, y], b_all.at[c, y], device))
    for step in range(1, rows):
        other = lax.rem(y + step, rows)
        share(a_all.at[c, x, other])
        share(c_all.at[c, x, other])
    for step in range(1, columns):
        share(b_all.at[c, y, lax.rem(x + step, columns)])
    for copy in waits:
        copy.wait_recv()
    for step in range(1, columns):
        other = lax.rem(x + step, columns)
        share(a_all.at[c, other])
        share(c_all.at[c, other])
    for step in range(1, rows):
        share(b_all.at[c, lax.rem(y + step, rows)])
    for copy in last:
        copy.wait_recv()
    mail.close()


def gather_all(dims, first, second, vector):
    planes, rows, columns, cores = dims
    copies = 3 * (planes - 1) + 3 * (rows - 1) + 3 * (columns - 1)
    copies += (cores - 1) * (3 + 3 * (rows - 1) + 3 * (columns - 1) + 1) + 8
    shapes = (
        (cores, columns, rows, planes) + first.shape,
        (cores, rows, columns, planes) + second.shape,
        (cores, columns, rows, planes) + vector.shape,
    )
    return pl.pallas_call(
        partial(gather_kernel, dims),
        out_shape=[jax.ShapeDtypeStruct(shape, jnp.float32) for shape in shapes],
        in_specs=[pl.BlockSpec(memory_space=pltpu.VMEM)] * 3,
        out_specs=[pl.BlockSpec(memory_space=pltpu.VMEM)] * 3,
        scratch_shapes=[
            pltpu.SemaphoreType.DMA((3,)),
            pltpu.SemaphoreType.DMA((copies,)),
            pltpu.SemaphoreType.DMA((copies,)),
        ],
        compiler_params=pltpu.CompilerParams(collective_id=0, has_side_effects=True),
        name="gather_weights",
    )(first, second, vector)


def split3(value):
    high = value.astype(jnp.bfloat16)
    return high, (value - high.astype(jnp.float32)).astype(jnp.bfloat16)


def dot3(left, right, dims=((1,), (0,))):
    def one(a, b):
        return lax.dot_general(a, b, (dims, ((), ())), preferred_element_type=jnp.float32)
    return one(left[0], right[0]) + (one(left[0], right[1]) + one(left[1], right[0]))


def tail_kernel(
    dims, owners,
    a_part, b_part, c_part, loss_ref, rate_ref, muon_w, muon_m, adam_w, adam_1, adam_2,
    new_w, new_m, new_a, new_1, new_2, scal_ref,
    a1, b1, c1, a2, b2, c2, a3, b3, c3, a4, b4, c4,
    ga, gb, gc, stat_out, stat_all, g_all, m_all, x_out, x_all,
    own_sems, send_sems, recv_sems, row_send, row_recv, x_send, x_recv, stat_send, stat_recv,
):
    planes, rows, columns, cores = dims
    z, y, x, c = spot = place_of(dims)
    mesh_count, pts_count = planes * rows, columns * cores
    count = mesh_count * pts_count
    me = lax.axis_index("mesh") * pts_count + lax.axis_index("pts")

    def device_of(number):
        return {"mesh": number // pts_count, "pts": lax.rem(number, pts_count)}

    barrier = pltpu.get_barrier_semaphore()

    @pl.loop(1, count)
    def _(step):
        pl.semaphore_signal(
            barrier, inc=1, device_id=device_of(lax.rem(me + step, count)), device_id_type=MESH
        )

    pl.semaphore_wait(barrier, count - 1)
    mats = len(owners)
    per = mats // 2
    def to_owner(k, source, table, slot):
        return pltpu.make_async_remote_copy(
            src_ref=source,
            dst_ref=table.at[me],
            send_sem=row_send.at[slot],
            recv_sem=row_recv.at[slot, me],
            device_id=device_of(owners[k]),
            device_id_type=MESH,
        )

    for k in range(mats):
        @pl.when(me != owners[k])
        def _():
            to_owner(k, muon_m.at[k], m_all, k).start()

        @pl.when(me == owners[k])
        def _():
            m_all[me] = muon_m[k]

    mail = Mail(send_sems, recv_sems)
    waits = []
    for step in range(1, cores):
        other = lax.rem(c + step, cores)
        device = device_at(dims, (z, y, x, other))
        for part, landing in ((a_part, a1), (b_part, b1), (c_part, c1)):
            waits.append(mail.send(part.at[other], landing.at[step - 1], device))
    for copy in waits:
        copy.wait_recv()
    for part, landing in ((a_part, a1), (b_part, b1), (c_part, c1)):
        total = part[c]
        for step in range(cores - 1):
            total = total + landing[step]
        landing[0] = total
    waits = []
    for step in range(1, columns):
        other = lax.rem(x + step, columns)
        device = device_at(dims, (z, y, other, c))
        waits.append(mail.send(a1.at[0, other], a2.at[step - 1], device))
        waits.append(mail.send(c1.at[0, other], c2.at[step - 1], device))
    for step in range(1, rows):
        other = lax.rem(y + step, rows)
        device = device_at(dims, (z, other, x, c))
        waits.append(mail.send(b1.at[0, other], b2.at[step - 1], device))
    for copy in waits:
        copy.wait_recv()
    for full, landing, at, extent in (
        (a1, a2, x, columns), (b1, b2, y, rows), (c1, c2, x, columns),
    ):
        total = full[0, at]
        for step in range(extent - 1):
            total = total + landing[step]
        landing[0] = total
    waits = []
    for step in range(1, rows):
        other = lax.rem(y + step, rows)
        device = device_at(dims, (z, other, x, c))
        waits.append(mail.send(a2.at[0, other], a3.at[step - 1], device))
        waits.append(mail.send(c2.at[0, other], c3.at[step - 1], device))
    for step in range(1, columns):
        other = lax.rem(x + step, columns)
        device = device_at(dims, (z, y, other, c))
        waits.append(mail.send(b2.at[0, other], b3.at[step - 1], device))
    for copy in waits:
        copy.wait_recv()
    for full, landing, at, extent in (
        (a2, a3, y, rows), (b2, b3, x, columns), (c2, c3, y, rows),
    ):
        total = full[0, at]
        for step in range(extent - 1):
            total = total + landing[step]
        landing[0] = total
    waits = []
    for step in range(1, planes):
        other = lax.rem(z + step, planes)
        device = device_at(dims, (other, y, x, c))
        for full, landing in ((a3, a4), (b3, b4), (c3, c4)):
            waits.append(mail.send(full.at[0, other], landing.at[step - 1], device))
    for copy in waits:
        copy.wait_recv()
    for full, landing, final in ((a3, a4, ga), (b3, b4, gb), (c3, c4, gc)):
        total = full[0, z]
        for step in range(planes - 1):
            total = total + landing[step]
        final[...] = total

    for k in range(mats):
        source = ga if k < per else gb

        @pl.when(me != owners[k])
        def _():
            to_owner(k, source.at[k % per], g_all, mats + k).start()

        @pl.when(me == owners[k])
        def _():
            g_all[me] = source[k % per]

    squares = jnp.sum(ga[...] * ga[...], axis=0) + jnp.sum(gb[...] * gb[...], axis=0)
    squares = squares + jnp.sum(gc[...] * gc[...], axis=0)
    square = jnp.sum(squares)
    lane = lax.broadcasted_iota(jnp.int32, (1, 128), 1)
    stat_out[...] = jnp.where(lane == 0, square, jnp.where(lane == 1, loss_ref[0], 0.0))
    stat_all[me] = stat_out[...]

    def stat_copy(step):
        return pltpu.make_async_remote_copy(
            src_ref=stat_out,
            dst_ref=stat_all.at[me],
            send_sem=stat_send.at[step],
            recv_sem=stat_recv.at[step],
            device_id=device_of(lax.rem(me + step, count)),
            device_id_type=MESH,
        )

    @pl.loop(1, count)
    def _(step):
        stat_copy(step).start()

    @pl.loop(1, count)
    def _(step):
        stat_copy(step).wait_recv()

    stats = jnp.sum(stat_all[...], axis=0)
    square_sum = jnp.sum(jnp.where(lane == 0, stats, 0.0))
    loss_sum = jnp.sum(jnp.where(lane == 1, stats, 0.0))
    norm = jnp.sqrt(jnp.full((8, 256), square_sum, jnp.float32))
    factor = 0.1 / jnp.maximum(norm, 0.1)
    row = lax.broadcasted_iota(jnp.int32, (8, 128), 0)
    scal_ref[...] = jnp.where(row == 0, norm[:, :128], jnp.full((8, 128), loss_sum, jnp.float32))

    for k in range(mats):
        @pl.when(me == owners[k])
        def _():
            for slot in (k, mats + k):
                table = m_all if slot < mats else g_all

                @pl.loop(1, count)
                def _(step):
                    source = lax.rem(me + step, count)
                    pltpu.make_async_remote_copy(
                        src_ref=muon_m.at[k],
                        dst_ref=table.at[source],
                        send_sem=row_send.at[slot],
                        recv_sem=row_recv.at[slot, source],
                        device_id=device_of(source),
                        device_id_type=MESH,
                    ).wait_recv()

            moment = 0.95 * m_all[...] + factor[None] * g_all[...]
            moment = moment.reshape(count * moment.shape[1], moment.shape[2])
            frob = jnp.sum(moment * moment)
            scale = jnp.sqrt(jnp.full((8, 256), frob, jnp.float32)) + 1e-07
            current = moment / scale[:1]
            for sweep in range(5):
                pair = split3(current)
                gram = split3(dot3(pair, pair, ((0,), (0,))))
                product = dot3(pair, gram)
                current = (
                    ns_a * current + ns_b * product + ns_c * dot3(split3(product), gram)
                )
            x_out[...] = current.reshape(x_out.shape)
            x_all[k] = x_out[me]

            @pl.loop(1, count)
            def _(step):
                target = lax.rem(me + step, count)
                pltpu.make_async_remote_copy(
                    src_ref=x_out.at[target],
                    dst_ref=x_all.at[k],
                    send_sem=x_send.at[target],
                    recv_sem=x_recv.at[k],
                    device_id=device_of(target),
                    device_id_type=MESH,
                ).start()

    new_m[:per] = 0.95 * muon_m[:per] + factor[None] * ga[...]
    new_m[per:] = 0.95 * muon_m[per:] + factor[None] * gb[...]
    rate, keep1, keep2 = rate_ref[0], rate_ref[1], rate_ref[2]
    clipped = factor[None] * gc[...]
    first = 0.9 * adam_1[...] + 0.1 * clipped
    second = 0.999 * adam_2[...] + 0.001 * clipped * clipped
    new_1[...] = first
    new_2[...] = second
    first_hat = first / keep1
    second_hat = second / keep2
    new_a[...] = adam_w[...] * (1.0 - rate * 0.01) - rate * first_hat / (
        jnp.sqrt(second_hat) + 1e-08
    )
    for k in range(mats):
        @pl.when(me != owners[k])
        def _():
            pltpu.make_async_remote_copy(
                src_ref=x_out.at[me],
                dst_ref=x_all.at[k],
                send_sem=x_send.at[me],
                recv_sem=x_recv.at[k],
                device_id=device_of(owners[k]),
                device_id_type=MESH,
            ).wait_recv()

    new_w[...] = muon_w[...] * (1.0 - rate * 0.01) - rate * (0.2 * C**0.5) * x_all[...]
    mail.close()

    @pl.loop(1, count)
    def _(step):
        stat_copy(step).wait_send()

    for k in range(mats):
        @pl.when(me != owners[k])
        def _():
            to_owner(k, muon_m.at[k], m_all, k).wait_send()
            to_owner(k, ga.at[k % per], g_all, mats + k).wait_send()

        @pl.when(me == owners[k])
        def _():
            @pl.loop(1, count)
            def _(step):
                target = lax.rem(me + step, count)
                pltpu.make_async_remote_copy(
                    src_ref=x_out.at[target],
                    dst_ref=x_all.at[k],
                    send_sem=x_send.at[target],
                    recv_sem=x_recv.at[k],
                    device_id=device_of(target),
                    device_id_type=MESH,
                ).wait_send()


def tail_update(dims, first, second, vector, loss, rates, muon_w, muon_m, adam_w, adam_1, adam_2):
    planes, rows, columns, cores = dims
    count = planes * rows * columns * cores
    mats = muon_m.shape[0]
    owners = tuple(k * count // mats for k in range(mats))
    blocks = (first.shape[4:], second.shape[4:], vector.shape[4:])
    orders = ((columns, rows, planes), (rows, columns, planes), (columns, rows, planes))
    landings = []
    for stage in range(4):
        for block, order, extents in zip(
            blocks, orders,
            ((cores, columns, rows, planes), (cores, rows, columns, planes), (cores, columns, rows, planes)),
        ):
            lead = max(extents[stage] - 1, 1)
            landings.append(pltpu.VMEM((lead,) + order[stage:] + block, jnp.float32))
    copies = 3 * (planes + rows + columns + cores)
    vmem = pl.BlockSpec(memory_space=pltpu.VMEM)
    smem = pl.BlockSpec(memory_space=pltpu.SMEM)
    dma = pltpu.SemaphoreType.DMA
    out = [muon_w, muon_m, adam_w, adam_1, adam_2]
    return pl.pallas_call(
        partial(tail_kernel, dims, owners),
        out_shape=[jax.ShapeDtypeStruct(item.shape, jnp.float32) for item in out]
        + [jax.ShapeDtypeStruct((8, 128), jnp.float32)],
        in_specs=[vmem] * 3 + [smem] * 2 + [vmem] * 5,
        out_specs=[vmem] * 6,
        scratch_shapes=landings
        + [
            pltpu.VMEM(blocks[0], jnp.float32),
            pltpu.VMEM(blocks[1], jnp.float32),
            pltpu.VMEM(blocks[2], jnp.float32),
            pltpu.VMEM((1, 128), jnp.float32),
            pltpu.VMEM((count, 1, 128), jnp.float32),
            pltpu.VMEM((count,) + muon_m.shape[1:], jnp.float32),
            pltpu.VMEM((count,) + muon_m.shape[1:], jnp.float32),
            pltpu.VMEM((count,) + muon_m.shape[1:], jnp.float32),
            pltpu.VMEM(muon_m.shape, jnp.float32),
            dma((1,)), dma((copies,)), dma((copies,)),
            dma((2 * mats,)), dma((2 * mats, count)), dma((count,)), dma((mats,)),
            dma((count,)), dma((count,)),
        ],
        compiler_params=pltpu.CompilerParams(
            collective_id=1, has_side_effects=True, vmem_limit_bytes=60 * 1024 * 1024
        ),
        name="reduce_and_update",
    )(first, second, vector, loss, rates, muon_w, muon_m, adam_w, adam_1, adam_2)


def local(
    inputs,
    target,
    lengths,
    step_count,
    muon_weight,
    muon_moment,
    adam_weight,
    adam_first,
    adam_second,
):
    muon_all, adam_all = (
        lax.all_gather(muon_weight, ("mesh", "pts"), axis=2, tiled=True),
        lax.all_gather(adam_weight, ("mesh", "pts"), axis=0, tiled=True),
    )
    points = inputs.shape[0]
    pts_count = lax.axis_size("pts")
    floor_value = float(points * pts_count)
    onehot = mesh_mask(lengths[0], lax.axis_index("pts") * points, points)
    meshes = lax.axis_size("mesh") * lengths.shape[1]
    hidden, embed_back = jax.vjp(lambda packed: embed_piece(inputs, packed), adam_all)
    saved = []
    for layer_index in range(L):
        matrices = muon_all[layer_index]
        (weights, numerator, denominator), slice_back = jax.vjp(
            partial(slice_piece, layer_index=layer_index, onehot=onehot), hidden, matrices, adam_all
        )
        numerator, denominator = lax.psum((numerator, denominator), "pts")
        mixed, mix_back = jax.vjp(
            partial(mix_piece, layer_index=layer_index), numerator, denominator, adam_all
        )
        following, out_back = jax.vjp(
            partial(out_piece, layer_index=layer_index, onehot=onehot),
            hidden,
            weights,
            mixed,
            matrices,
            adam_all,
        )
        saved.append((slice_back, mix_back, out_back))
        hidden = following
    (errors, scales), head_back = jax.vjp(
        lambda state, packed: head_piece(state, packed, target, onehot), hidden, adam_all
    )
    errors, scales = lax.psum((errors, scales), "pts")
    group_loss, loss_back = jax.vjp(
        lambda first, second: loss_piece(first, second, meshes, floor_value), errors, scales
    )
    grad_errors, grad_scales = loss_back(jnp.ones_like(group_loss))
    grad_hidden, grad_adam = head_back((grad_errors, grad_scales))
    grad_layers = [None] * L
    for layer_index in reversed(range(L)):
        slice_back, mix_back, out_back = saved[layer_index]
        grad_hidden_out, grad_weights, grad_mixed, grad_mats_out, grad_adam_out = out_back(
            grad_hidden
        )
        grad_mixed = lax.psum(grad_mixed, "pts")
        grad_num, grad_den, grad_adam_mix = mix_back(grad_mixed)
        grad_hidden_in, grad_mats_in, grad_adam_in = slice_back((grad_weights, grad_num, grad_den))
        grad_hidden = grad_hidden_out + grad_hidden_in
        grad_adam = grad_adam + grad_adam_out + grad_adam_in + grad_adam_mix / pts_count
        grad_layers[layer_index] = grad_mats_out + grad_mats_in
    (grad_embed,) = embed_back(grad_hidden)
    grad_adam = grad_adam + grad_embed
    grad_muon = jnp.stack(grad_layers)
    grad_muon, grad_adam = (
        lax.psum_scatter(grad_muon, ("mesh", "pts"), scatter_dimension=2, tiled=True),
        lax.psum_scatter(grad_adam, ("mesh", "pts"), scatter_dimension=0, tiled=True),
    )
    square_sum, loss_total = lax.psum(
        (jnp.sum(grad_muon * grad_muon) + jnp.sum(grad_adam * grad_adam), group_loss / pts_count),
        ("mesh", "pts"),
    )

    def frob_of(moment):
        return lax.psum(jnp.sum(moment * moment, axis=(2, 3)), ("mesh", "pts"))

    def orthogonal_of(normalized):
        groups = lax.axis_size("mesh")
        count_all = normalized.shape[0] * normalized.shape[1]
        per_group = (count_all + groups - 1) // groups
        stacked = normalized.reshape((count_all,) + normalized.shape[2:])
        filler = jnp.zeros((per_group * groups - count_all,) + normalized.shape[2:], jnp.float32)
        spread = lax.all_to_all(
            jnp.concatenate([stacked, filler], axis=0),
            "mesh",
            split_axis=0,
            concat_axis=1,
            tiled=True,
        )

        def gram_of(current):
            return lax.psum(jnp.einsum("krc,krd->kcd", current, current, precision=HIGH), "pts")

        finished = newton_schulz(spread, gram_of)
        returned = lax.all_to_all(finished, "mesh", split_axis=1, concat_axis=0, tiled=True)
        return returned[:count_all].reshape(normalized.shape)

    results = apply_update(
        grad_muon,
        grad_adam,
        square_sum,
        step_count,
        muon_weight,
        muon_moment,
        adam_weight,
        adam_first,
        adam_second,
        frob_of,
        orthogonal_of,
    )
    return (results[0], results[1], results[2], results[3], results[4], loss_total, results[5])


def local_fast(
    inputs,
    target,
    lengths,
    step_count,
    muon_weight,
    muon_moment,
    adam_weight,
    adam_first,
    adam_second,
):
    mesh_count, pts_count = lax.axis_size("mesh"), lax.axis_size("pts")
    dims = grid_of(mesh_count, pts_count)
    planes, rows, columns, cores = dims
    count = mesh_count * pts_count
    shard, span = adam_weight.shape[0], muon_weight.shape[2]
    mats = muon_weight.shape[0] * muon_weight.shape[1]
    slabs = span // 8
    pad = -(-shard // 2048) * 2048

    def slab_of(vector):
        return jnp.pad(vector, (0, pad - shard)).reshape(-1, 8, 256)

    def stacked(value):
        return value.reshape(mats * slabs, 8, 256)

    half = muon_weight.shape[1] * slabs
    all_first, all_second, all_vector = gather_all(
        dims, muon_weight[0].reshape(half, 8, 256), muon_weight[1].reshape(half, 8, 256), slab_of(adam_weight)
    )

    def matrices_of(value, order):
        value = value.reshape(value.shape[:4] + (half // slabs, slabs, 8, 256))
        value = jnp.transpose(value, (4,) + order + (5, 6, 7))
        return value.reshape(half // slabs, count * span, 256)

    muon_all = (
        matrices_of(all_first, (3, 2, 1, 0)), matrices_of(all_second, (3, 1, 2, 0))
    )
    adam_all = jnp.transpose(all_vector, (3, 2, 1, 0, 4, 5, 6)).reshape(count, pad)[:, :shard].reshape(-1)
    points = inputs.shape[0]
    pts_count = lax.axis_size("pts")
    floor_value = float(points * pts_count)
    onehot = mesh_mask(lengths[0], lax.axis_index("pts") * points, points)
    meshes = lax.axis_size("mesh") * lengths.shape[1]
    hidden, embed_back = jax.vjp(lambda packed: embed_piece(inputs, packed), adam_all)
    saved = []
    for layer_index in range(L):
        matrices = muon_all[layer_index]
        (weights, numerator, denominator), slice_back = jax.vjp(
            partial(slice_piece, layer_index=layer_index, onehot=onehot), hidden, matrices, adam_all
        )
        numerator, denominator = lax.psum((numerator, denominator), "pts")
        mixed, mix_back = jax.vjp(
            partial(mix_piece, layer_index=layer_index), numerator, denominator, adam_all
        )
        following, out_back = jax.vjp(
            partial(out_piece, layer_index=layer_index, onehot=onehot),
            hidden,
            weights,
            mixed,
            matrices,
            adam_all,
        )
        saved.append((slice_back, mix_back, out_back))
        hidden = following
    (errors, scales), head_back = jax.vjp(
        lambda state, packed: head_piece(state, packed, target, onehot), hidden, adam_all
    )
    errors, scales = lax.psum((errors, scales), "pts")
    group_loss, loss_back = jax.vjp(
        lambda first, second: loss_piece(first, second, meshes, floor_value), errors, scales
    )
    grad_errors, grad_scales = loss_back(jnp.ones_like(group_loss))
    grad_hidden, grad_adam = head_back((grad_errors, grad_scales))
    grad_layers = [None] * L
    for layer_index in reversed(range(L)):
        slice_back, mix_back, out_back = saved[layer_index]
        grad_hidden_out, grad_weights, grad_mixed, grad_mats_out, grad_adam_out = out_back(
            grad_hidden
        )
        grad_mixed = lax.psum(grad_mixed, "pts")
        grad_num, grad_den, grad_adam_mix = mix_back(grad_mixed)
        grad_hidden_in, grad_mats_in, grad_adam_in = slice_back((grad_weights, grad_num, grad_den))
        grad_hidden = grad_hidden_out + grad_hidden_in
        grad_adam = grad_adam + grad_adam_out + grad_adam_in + grad_adam_mix / pts_count
        grad_layers[layer_index] = grad_mats_out + grad_mats_in
    (grad_embed,) = embed_back(grad_hidden)
    grad_adam = grad_adam + grad_embed
    def parts_of(value, order):
        value = value.reshape(half // slabs, planes, rows, columns, cores, slabs, 8, 256)
        value = jnp.transpose(value, order + (0, 5, 6, 7))
        return value.reshape(value.shape[:4] + (half, 8, 256))

    adam_parts = jnp.pad(grad_adam.reshape(count, shard), ((0, 0), (0, pad - shard)))
    adam_parts = adam_parts.reshape(planes, rows, columns, cores, -1, 8, 256)
    adam_parts = jnp.transpose(adam_parts, (3, 2, 1, 0, 4, 5, 6))
    step = step_count[0].astype(jnp.float32)
    rates = jnp.stack([one_cycle(step), 1.0 - 0.9**step, 1.0 - 0.999**step])
    results = tail_update(
        dims,
        parts_of(grad_layers[0], (4, 3, 2, 1)),
        parts_of(grad_layers[1], (4, 2, 3, 1)),
        adam_parts,
        jnp.reshape(group_loss / pts_count, (1,)),
        rates,
        stacked(muon_weight),
        stacked(muon_moment),
        slab_of(adam_weight),
        slab_of(adam_first),
        slab_of(adam_second),
    )

    def unslab(value):
        return value.reshape(-1)[:shard]

    return (
        results[0].reshape(muon_weight.shape),
        results[1].reshape(muon_weight.shape),
        unslab(results[2]),
        unslab(results[3]),
        unslab(results[4]),
        results[5][1, 0],
        results[5][0, 0],
    )


def solution(mesh):
    in_specs = (
        P(("mesh", "pts"), None),
        P(("mesh", "pts"), None),
        P("mesh", None),
        P(),
        P(None, None, ("mesh", "pts"), None),
        P(None, None, ("mesh", "pts"), None),
        P(("mesh", "pts")),
        P(("mesh", "pts")),
        P(("mesh", "pts")),
    )
    out_specs = (
        P(None, None, ("mesh", "pts"), None),
        P(None, None, ("mesh", "pts"), None),
        P(("mesh", "pts")),
        P(("mesh", "pts")),
        P(("mesh", "pts")),
        P(),
        P(),
    )
    def chosen(*args):
        return (local_fast if args[4].shape[2] == 8 else local)(*args)

    return jax.shard_map(chosen, mesh=mesh, in_specs=in_specs, out_specs=out_specs, check_vma=False)
```

```python
from functools import partial
import math

import jax
import jax.numpy as jnp
from jax import lax
from jax.experimental import pallas as pl
from jax.experimental.pallas import tpu as pltpu
from jax.sharding import PartitionSpec as P

C = 256
H = 8
DH = 32
S = 64
IN = 8
OUT = 4
L = 2


HIGH = lax.Precision.HIGH
ns_a = 3.4445
ns_b = -4.775
ns_c = 2.0315
peak_rate = 0.3
warm_steps = 12.0
total_steps = 40.0


def layout():
    pieces = [
        ("emb_w", (IN, C)),
        ("emb_b", (C,)),
        ("head_w", (C, OUT)),
        ("head_b", (OUT,)),
        ("fin", (2, C)),
        ("qkv", (L, 3, DH, DH)),
        ("slice_w", (L, DH, S)),
        ("slice_b", (L, S)),
        ("temp", (L, H)),
        ("vec", (L, 9, C)),
    ]
    places = {}
    offset = 0
    for label_text, extent in pieces:
        places[label_text] = (offset, extent)
        offset = offset + math.prod(extent)
    return places


def unpack(packed):
    return {
        label_text: packed[offset : offset + math.prod(extent)].reshape(extent)
        for label_text, (offset, extent) in layout().items()
    }


def matmul(left, right):
    return jnp.dot(left, right, precision=HIGH)


def norm_rows(values, gain, shift):
    centre = values - jnp.mean(values, axis=-1, keepdims=True)
    spread = jnp.mean(centre * centre, axis=-1, keepdims=True)
    return centre * lax.rsqrt(spread + 1e-05) * gain + shift


def mesh_mask(lengths_row, first, points):
    ends = jnp.cumsum(lengths_row)
    starts = ends - lengths_row
    position = first + jnp.arange(points, dtype=jnp.int32)
    inside = (position[:, None] >= starts[None, :]) & (position[:, None] < ends[None, :])
    return inside.astype(jnp.float32)


def embed_piece(inputs, packed):
    params = unpack(packed)
    return matmul(inputs, params["emb_w"]) + params["emb_b"]


def slice_piece(hidden, matrices, packed, layer_index, onehot):
    params = unpack(packed)
    vectors = params["vec"][layer_index]
    points = hidden.shape[0]
    normed = norm_rows(hidden, vectors[0], vectors[1])
    features = (matmul(normed, matrices[0]) + vectors[2]).reshape(points, H, DH)
    routed = (matmul(normed, matrices[1]) + vectors[3]).reshape(points, H, DH)
    logits = jnp.einsum("phd,ds->phs", routed, params["slice_w"][layer_index], precision=HIGH)
    logits = (logits + params["slice_b"][layer_index]) / params["temp"][layer_index][:, None]
    weights = jax.nn.softmax(logits, axis=-1)
    numerator = jnp.einsum("pm,phs,phd->mhsd", onehot, weights, features, precision=HIGH)
    denominator = jnp.einsum("pm,phs->mhs", onehot, weights, precision=HIGH)
    return (weights, numerator, denominator)


def mix_piece(numerator, denominator, packed, layer_index):
    triple = unpack(packed)["qkv"][layer_index]
    tokens = numerator / (denominator[..., None] + 1e-05)
    queries = jnp.einsum("mhsd,de->mhse", tokens, triple[0], precision=HIGH)
    keys_all = jnp.einsum("mhsd,de->mhse", tokens, triple[1], precision=HIGH)
    values = jnp.einsum("mhsd,de->mhse", tokens, triple[2], precision=HIGH)
    scores = jnp.einsum("mhsd,mhtd->mhst", queries, keys_all, precision=HIGH) * DH ** (-0.5)
    return jnp.einsum("mhst,mhtd->mhsd", jax.nn.softmax(scores, axis=-1), values, precision=HIGH)


def out_piece(hidden, weights, mixed, matrices, packed, layer_index, onehot):
    vectors = unpack(packed)["vec"][layer_index]
    points = hidden.shape[0]
    spread_wts = onehot[:, :, None, None] * weights[:, None, :, :]
    pointwise = jnp.einsum("pmhs,mhsd->phd", spread_wts, mixed, precision=HIGH).reshape(points, C)
    hidden = hidden + matmul(pointwise, matrices[2]) + vectors[4]
    normed = norm_rows(hidden, vectors[5], vectors[6])
    inner = jax.nn.gelu(matmul(normed, matrices[3]) + vectors[7], approximate=False)
    return hidden + matmul(inner, matrices[4]) + vectors[8]


def head_piece(hidden, packed, target, onehot):
    params = unpack(packed)
    normed = norm_rows(hidden, params["fin"][0], params["fin"][1])
    predicted = matmul(normed, params["head_w"]) + params["head_b"]
    misfit = predicted - target
    errors = matmul(onehot.T, jnp.sum(misfit * misfit, axis=-1))
    scales = matmul(onehot.T, jnp.sum(target * target, axis=-1))
    return (errors, scales)


def loss_piece(errors, scales, meshes, floor_value):
    return jnp.sum(jnp.sqrt((errors + 1e-06) / jnp.maximum(scales, floor_value))) / meshes


def one_cycle(count):
    start_rate = peak_rate / 25.0
    end_rate = start_rate / 10000.0
    rising = start_rate + (peak_rate - start_rate) * 0.5 * (
        1.0 - jnp.cos(math.pi * count / warm_steps)
    )
    falling = end_rate + (peak_rate - end_rate) * 0.5 * (
        1.0 + jnp.cos(math.pi * (count - warm_steps) / (total_steps - warm_steps))
    )
    return jnp.where(count <= warm_steps, rising, falling)


def newton_schulz(current, gram_of):
    for sweep in range(5):
        gram = gram_of(current)
        product = jnp.einsum("...rc,...cd->...rd", current, gram, precision=HIGH)
        current = (
            ns_a * current
            + ns_b * product
            + ns_c * jnp.einsum("...rc,...cd->...rd", product, gram, precision=HIGH)
        )
    return current


def apply_update(
    grad_muon,
    grad_adam,
    square_sum,
    step_count,
    muon_weight,
    muon_moment,
    adam_weight,
    adam_first,
    adam_second,
    frob_of,
    orthogonal_of,
):
    norm_value = jnp.sqrt(square_sum)
    factor = 0.1 / jnp.maximum(norm_value, 0.1)
    moment = 0.95 * muon_moment + factor * grad_muon
    normalized = moment / (jnp.sqrt(frob_of(moment)) + 1e-07)[..., None, None]
    current = orthogonal_of(normalized)
    count = step_count[0].astype(jnp.float32)
    rate = one_cycle(count)
    new_muon = muon_weight * (1.0 - rate * 0.01) - rate * (0.2 * C**0.5) * current
    clipped = factor * grad_adam
    first = 0.9 * adam_first + 0.1 * clipped
    second = 0.999 * adam_second + 0.001 * clipped * clipped
    first_hat = first / (1.0 - 0.9**count)
    second_hat = second / (1.0 - 0.999**count)
    new_adam = adam_weight * (1.0 - rate * 0.01) - rate * first_hat / (jnp.sqrt(second_hat) + 1e-08)
    return (new_muon, moment, new_adam, first, second, norm_value)


MESH = pl.DeviceIdType.MESH
SLAB = (8, 256)


def grid_of(mesh_count, pts_count):
    cores = 2 if pts_count % 2 == 0 else 1
    rows = max(math.isqrt(mesh_count // 2), 1)
    while mesh_count % rows:
        rows -= 1
    return mesh_count // rows, rows, pts_count // cores, cores


def place_of(dims):
    planes, rows, columns, cores = dims
    across, along = lax.axis_index("mesh"), lax.axis_index("pts")
    return across // rows, across % rows, along // cores, along % cores


def device_at(dims, spot):
    z, y, x, c = spot
    return {"mesh": z * dims[1] + y, "pts": x * dims[3] + c}


def line_partners(dims, spot):
    found = []
    for axis in range(4):
        for step in range(1, dims[axis]):
            other = list(spot)
            other[axis] = lax.rem(spot[axis] + step, dims[axis])
            found.append(device_at(dims, other))
    return found


def greet(partners):
    barrier = pltpu.get_barrier_semaphore()
    for partner in partners:
        pl.semaphore_signal(barrier, inc=1, device_id=partner, device_id_type=MESH)
    pl.semaphore_wait(barrier, len(partners))


class Mail:
    def __init__(self, send_sems, recv_sems):
        self.send_sems, self.recv_sems, self.used, self.open = send_sems, recv_sems, 0, []

    def send(self, source, target, device):
        copy = pltpu.make_async_remote_copy(
            src_ref=source,
            dst_ref=target,
            send_sem=self.send_sems.at[self.used],
            recv_sem=self.recv_sems.at[self.used],
            device_id=device,
            device_id_type=MESH,
        )
        copy.start()
        self.used += 1
        self.open.append(copy)
        return copy

    def close(self):
        for copy in self.open:
            copy.wait_send()


def gather_kernel(dims, a_in, b_in, c_in, a_all, b_all, c_all, keep, send_sems, recv_sems):
    planes, rows, columns, cores = dims
    z, y, x, c = spot = place_of(dims)
    own = []
    for index, (source, target) in enumerate(
        ((a_in, a_all.at[c, x, y, z]), (b_in, b_all.at[c, y, x, z]), (c_in, c_all.at[c, x, y, z]))
    ):
        copy = pltpu.make_async_copy(source, target, keep.at[index])
        copy.start()
        own.append(copy)
    greet(line_partners(dims, spot))
    mail = Mail(send_sems, recv_sems)
    waits = []
    for step in range(1, planes):
        device = device_at(dims, (lax.rem(z + step, planes), y, x, c))
        waits.append(mail.send(a_in, a_all.at[c, x, y, z], device))
        waits.append(mail.send(b_in, b_all.at[c, y, x, z], device))
        waits.append(mail.send(c_in, c_all.at[c, x, y, z], device))
    for copy in own:
        copy.wait()
    for copy in waits:
        copy.wait_recv()
    partner = [device_at(dims, (z, y, x, lax.rem(c + step, cores))) for step in range(1, cores)]
    last = []

    def share(reference):
        for device in partner:
            last.append(mail.send(reference, reference, device))

    waits = []
    for step in range(1, rows):
        device = device_at(dims, (z, lax.rem(y + step, rows), x, c))
        for full in (a_all, c_all):
            waits.append(mail.send(full.at[c, x, y], full.at[c, x, y], device))
    for step in range(1, columns):
        device = device_at(dims, (z, y, lax.rem(x + step, columns), c))
        waits.append(mail.send(b_all.at[c, y, x], b_all.at[c, y, x], device))
    for reference in (a_all.at[c, x, y], b_all.at[c, y, x], c_all.at[c, x, y]):
        share(reference)
    for copy in waits:
        copy.wait_recv()
    waits = []
    for step in range(1, columns):
        device = device_at(dims, (z, y, lax.rem(x + step, columns), c))
        for full in (a_all, c_all):
            waits.append(mail.send(full.at[c, x], full.at[c, x], device))
    for step in range(1, rows):
        device = device_at(dims, (z, lax.rem(y + step, rows), x, c))
        waits.append(mail.send(b_all.at[c, y], b_all.at[c, y], device))
    for step in range(1, rows):
        other = lax.rem(y + step, rows)
        share(a_all.at[c, x, other])
        share(c_all.at[c, x, other])
    for step in range(1, columns):
        share(b_all.at[c, y, lax.rem(x + step, columns)])
    for copy in waits:
        copy.wait_recv()
    for step in range(1, columns):
        other = lax.rem(x + step, columns)
        share(a_all.at[c, other])
        share(c_all.at[c, other])
    for step in range(1, rows):
        share(b_all.at[c, lax.rem(y + step, rows)])
    for copy in last:
        copy.wait_recv()
    mail.close()


def gather_all(dims, first, second, vector):
    planes, rows, columns, cores = dims
    copies = 3 * (planes - 1) + 3 * (rows - 1) + 3 * (columns - 1)
    copies += (cores - 1) * (3 + 3 * (rows - 1) + 3 * (columns - 1) + 1) + 8
    shapes = (
        (cores, columns, rows, planes) + first.shape,
        (cores, rows, columns, planes) + second.shape,
        (cores, columns, rows, planes) + vector.shape,
    )
    return pl.pallas_call(
        partial(gather_kernel, dims),
        out_shape=[jax.ShapeDtypeStruct(shape, jnp.float32) for shape in shapes],
        in_specs=[pl.BlockSpec(memory_space=pltpu.VMEM)] * 3,
        out_specs=[pl.BlockSpec(memory_space=pltpu.VMEM)] * 3,
        scratch_shapes=[
            pltpu.SemaphoreType.DMA((3,)),
            pltpu.SemaphoreType.DMA((copies,)),
            pltpu.SemaphoreType.DMA((copies,)),
        ],
        compiler_params=pltpu.CompilerParams(collective_id=0, has_side_effects=True),
        name="gather_weights",
    )(first, second, vector)


def split3(value):
    high = value.astype(jnp.bfloat16)
    return high, (value - high.astype(jnp.float32)).astype(jnp.bfloat16)


def dot3(left, right, dims=((1,), (0,))):
    def one(a, b):
        return lax.dot_general(a, b, (dims, ((), ())), preferred_element_type=jnp.float32)
    return one(left[0], right[0]) + (one(left[0], right[1]) + one(left[1], right[0]))


def tail_kernel(
    dims, owners,
    a_part, b_part, c_part, loss_ref, rate_ref, muon_w, muon_m, adam_w, adam_1, adam_2,
    new_w, new_m, new_a, new_1, new_2, scal_ref,
    a1, b1, c1, a2, b2, c2, a3, b3, c3, a4, b4, c4,
    ga, gb, gc, stat_out, stat_all, g_all, m_all, x_out, x_all,
    own_sems, send_sems, recv_sems, row_send, row_recv, x_send, x_recv, stat_send, stat_recv,
):
    planes, rows, columns, cores = dims
    z, y, x, c = spot = place_of(dims)
    mesh_count, pts_count = planes * rows, columns * cores
    count = mesh_count * pts_count
    me = lax.axis_index("mesh") * pts_count + lax.axis_index("pts")

    def device_of(number):
        return {"mesh": number // pts_count, "pts": lax.rem(number, pts_count)}

    barrier = pltpu.get_barrier_semaphore()

    @pl.loop(1, count)
    def _(step):
        pl.semaphore_signal(
            barrier, inc=1, device_id=device_of(lax.rem(me + step, count)), device_id_type=MESH
        )

    pl.semaphore_wait(barrier, count - 1)
    mats = len(owners)
    per = mats // 2
    def to_owner(k, source, table, slot):
        return pltpu.make_async_remote_copy(
            src_ref=source,
            dst_ref=table.at[me],
            send_sem=row_send.at[slot],
            recv_sem=row_recv.at[slot, me],
            device_id=device_of(owners[k]),
            device_id_type=MESH,
        )

    for k in range(mats):
        @pl.when(me != owners[k])
        def _():
            to_owner(k, muon_m.at[k], m_all, k).start()

        @pl.when(me == owners[k])
        def _():
            m_all[me] = muon_m[k]

    mail = Mail(send_sems, recv_sems)
    waits = []
    for step in range(1, cores):
        other = lax.rem(c + step, cores)
        device = device_at(dims, (z, y, x, other))
        for part, landing in ((a_part, a1), (b_part, b1), (c_part, c1)):
            waits.append(mail.send(part.at[other], landing.at[step - 1], device))
    for copy in waits:
        copy.wait_recv()
    for part, landing in ((a_part, a1), (b_part, b1), (c_part, c1)):
        total = part[c]
        for step in range(cores - 1):
            total = total + landing[step]
        landing[0] = total
    waits = []
    for step in range(1, columns):
        other = lax.rem(x + step, columns)
        device = device_at(dims, (z, y, other, c))
        waits.append(mail.send(a1.at[0, other], a2.at[step - 1], device))
        waits.append(mail.send(c1.at[0, other], c2.at[step - 1], device))
    for step in range(1, rows):
        other = lax.rem(y + step, rows)
        device = device_at(dims, (z, other, x, c))
        waits.append(mail.send(b1.at[0, other], b2.at[step - 1], device))
    for copy in waits:
        copy.wait_recv()
    for full, landing, at, extent in (
        (a1, a2, x, columns), (b1, b2, y, rows), (c1, c2, x, columns),
    ):
        total = full[0, at]
        for step in range(extent - 1):
            total = total + landing[step]
        landing[0] = total
    waits = []
    for step in range(1, rows):
        other = lax.rem(y + step, rows)
        device = device_at(dims, (z, other, x, c))
        waits.append(mail.send(a2.at[0, other], a3.at[step - 1], device))
        waits.append(mail.send(c2.at[0, other], c3.at[step - 1], device))
    for step in range(1, columns):
        other = lax.rem(x + step, columns)
        device = device_at(dims, (z, y, other, c))
        waits.append(mail.send(b2.at[0, other], b3.at[step - 1], device))
    for copy in waits:
        copy.wait_recv()
    for full, landing, at, extent in (
        (a2, a3, y, rows), (b2, b3, x, columns), (c2, c3, y, rows),
    ):
        total = full[0, at]
        for step in range(extent - 1):
            total = total + landing[step]
        landing[0] = total
    waits = []
    for step in range(1, planes):
        other = lax.rem(z + step, planes)
        device = device_at(dims, (other, y, x, c))
        for full, landing in ((a3, a4), (b3, b4), (c3, c4)):
            waits.append(mail.send(full.at[0, other], landing.at[step - 1], device))
    for copy in waits:
        copy.wait_recv()
    for full, landing, final in ((a3, a4, ga), (b3, b4, gb), (c3, c4, gc)):
        total = full[0, z]
        for step in range(planes - 1):
            total = total + landing[step]
        final[...] = total

    for k in range(mats):
        source = ga if k < per else gb

        @pl.when(me != owners[k])
        def _():
            to_owner(k, source.at[k % per], g_all, mats + k).start()

        @pl.when(me == owners[k])
        def _():
            g_all[me] = source[k % per]

    squares = jnp.sum(ga[...] * ga[...], axis=0) + jnp.sum(gb[...] * gb[...], axis=0)
    squares = squares + jnp.sum(gc[...] * gc[...], axis=0)
    square = jnp.sum(squares)
    lane = lax.broadcasted_iota(jnp.int32, (1, 128), 1)
    stat_out[...] = jnp.where(lane == 0, square, jnp.where(lane == 1, loss_ref[0], 0.0))
    stat_all[me] = stat_out[...]

    def stat_copy(step):
        return pltpu.make_async_remote_copy(
            src_ref=stat_out,
            dst_ref=stat_all.at[me],
            send_sem=stat_send.at[step],
            recv_sem=stat_recv.at[step],
            device_id=device_of(lax.rem(me + step, count)),
            device_id_type=MESH,
        )

    @pl.loop(1, count)
    def _(step):
        stat_copy(step).start()

    @pl.loop(1, count)
    def _(step):
        stat_copy(step).wait_recv()

    stats = jnp.sum(stat_all[...], axis=0)
    square_sum = jnp.sum(jnp.where(lane == 0, stats, 0.0))
    loss_sum = jnp.sum(jnp.where(lane == 1, stats, 0.0))
    norm = jnp.sqrt(jnp.full((8, 256), square_sum, jnp.float32))
    factor = 0.1 / jnp.maximum(norm, 0.1)
    row = lax.broadcasted_iota(jnp.int32, (8, 128), 0)
    scal_ref[...] = jnp.where(row == 0, norm[:, :128], jnp.full((8, 128), loss_sum, jnp.float32))

    for k in range(mats):
        @pl.when(me == owners[k])
        def _():
            for slot in (k, mats + k):
                table = m_all if slot < mats else g_all

                @pl.loop(1, count)
                def _(step):
                    source = lax.rem(me + step, count)
                    pltpu.make_async_remote_copy(
                        src_ref=muon_m.at[k],
                        dst_ref=table.at[source],
                        send_sem=row_send.at[slot],
                        recv_sem=row_recv.at[slot, source],
                        device_id=device_of(source),
                        device_id_type=MESH,
                    ).wait_recv()

            moment = 0.95 * m_all[...] + factor[None] * g_all[...]
            moment = moment.reshape(count * moment.shape[1], moment.shape[2])
            frob = jnp.sum(moment * moment)
            scale = jnp.sqrt(jnp.full((8, 256), frob, jnp.float32)) + 1e-07
            current = moment / scale[:1]
            for sweep in range(5):
                pair = split3(current)
                gram = split3(dot3(pair, pair, ((0,), (0,))))
                product = dot3(pair, gram)
                current = (
                    ns_a * current + ns_b * product + ns_c * dot3(split3(product), gram)
                )
            x_out[...] = current.reshape(x_out.shape)
            x_all[k] = x_out[me]

            @pl.loop(1, count)
            def _(step):
                target = lax.rem(me + step, count)
                pltpu.make_async_remote_copy(
                    src_ref=x_out.at[target],
                    dst_ref=x_all.at[k],
                    send_sem=x_send.at[target],
                    recv_sem=x_recv.at[k],
                    device_id=device_of(target),
                    device_id_type=MESH,
                ).start()

    new_m[:per] = 0.95 * muon_m[:per] + factor[None] * ga[...]
    new_m[per:] = 0.95 * muon_m[per:] + factor[None] * gb[...]
    rate, keep1, keep2 = rate_ref[0], rate_ref[1], rate_ref[2]
    clipped = factor[None] * gc[...]
    first = 0.9 * adam_1[...] + 0.1 * clipped
    second = 0.999 * adam_2[...] + 0.001 * clipped * clipped
    new_1[...] = first
    new_2[...] = second
    first_hat = first / keep1
    second_hat = second / keep2
    new_a[...] = adam_w[...] * (1.0 - rate * 0.01) - rate * first_hat / (
        jnp.sqrt(second_hat) + 1e-08
    )
    for k in range(mats):
        @pl.when(me != owners[k])
        def _():
            pltpu.make_async_remote_copy(
                src_ref=x_out.at[me],
                dst_ref=x_all.at[k],
                send_sem=x_send.at[me],
                recv_sem=x_recv.at[k],
                device_id=device_of(owners[k]),
                device_id_type=MESH,
            ).wait_recv()

    new_w[...] = muon_w[...] * (1.0 - rate * 0.01) - rate * (0.2 * C**0.5) * x_all[...]
    mail.close()

    @pl.loop(1, count)
    def _(step):
        stat_copy(step).wait_send()

    for k in range(mats):
        @pl.when(me != owners[k])
        def _():
            to_owner(k, muon_m.at[k], m_all, k).wait_send()
            to_owner(k, ga.at[k % per], g_all, mats + k).wait_send()

        @pl.when(me == owners[k])
        def _():
            @pl.loop(1, count)
            def _(step):
                target = lax.rem(me + step, count)
                pltpu.make_async_remote_copy(
                    src_ref=x_out.at[target],
                    dst_ref=x_all.at[k],
                    send_sem=x_send.at[target],
                    recv_sem=x_recv.at[k],
                    device_id=device_of(target),
                    device_id_type=MESH,
                ).wait_send()


def tail_update(dims, first, second, vector, loss, rates, muon_w, muon_m, adam_w, adam_1, adam_2):
    planes, rows, columns, cores = dims
    count = planes * rows * columns * cores
    mats = muon_m.shape[0]
    owners = tuple(k * count // mats for k in range(mats))
    blocks = (first.shape[4:], second.shape[4:], vector.shape[4:])
    orders = ((columns, rows, planes), (rows, columns, planes), (columns, rows, planes))
    landings = []
    for stage in range(4):
        for block, order, extents in zip(
            blocks, orders,
            ((cores, columns, rows, planes), (cores, rows, columns, planes), (cores, columns, rows, planes)),
        ):
            lead = max(extents[stage] - 1, 1)
            landings.append(pltpu.VMEM((lead,) + order[stage:] + block, jnp.float32))
    copies = 3 * (planes + rows + columns + cores)
    vmem = pl.BlockSpec(memory_space=pltpu.VMEM)
    smem = pl.BlockSpec(memory_space=pltpu.SMEM)
    dma = pltpu.SemaphoreType.DMA
    out = [muon_w, muon_m, adam_w, adam_1, adam_2]
    return pl.pallas_call(
        partial(tail_kernel, dims, owners),
        out_shape=[jax.ShapeDtypeStruct(item.shape, jnp.float32) for item in out]
        + [jax.ShapeDtypeStruct((8, 128), jnp.float32)],
        in_specs=[vmem] * 3 + [smem] * 2 + [vmem] * 5,
        out_specs=[vmem] * 6,
        scratch_shapes=landings
        + [
            pltpu.VMEM(blocks[0], jnp.float32),
            pltpu.VMEM(blocks[1], jnp.float32),
            pltpu.VMEM(blocks[2], jnp.float32),
            pltpu.VMEM((1, 128), jnp.float32),
            pltpu.VMEM((count, 1, 128), jnp.float32),
            pltpu.VMEM((count,) + muon_m.shape[1:], jnp.float32),
            pltpu.VMEM((count,) + muon_m.shape[1:], jnp.float32),
            pltpu.VMEM((count,) + muon_m.shape[1:], jnp.float32),
            pltpu.VMEM(muon_m.shape, jnp.float32),
            dma((1,)), dma((copies,)), dma((copies,)),
            dma((2 * mats,)), dma((2 * mats, count)), dma((count,)), dma((mats,)),
            dma((count,)), dma((count,)),
        ],
        compiler_params=pltpu.CompilerParams(
            collective_id=1, has_side_effects=True, vmem_limit_bytes=60 * 1024 * 1024
        ),
        name="reduce_and_update",
    )(first, second, vector, loss, rates, muon_w, muon_m, adam_w, adam_1, adam_2)


TILE = 256
VMEM_CAP = 56 * 1024 * 1024


def pair(value):
    return split3(value)


NN = ((1,), (0,))
NT = ((1,), (1,))
TN = ((0,), (0,))


def normed_of(value):
    centre = value - jnp.mean(value, axis=0, keepdims=True)
    scale = lax.rsqrt(jnp.mean(centre * centre, axis=0, keepdims=True) + 1e-05)
    return centre * scale, scale


def norm_back(grad_hat, hat, scale):
    first = jnp.mean(grad_hat, axis=0, keepdims=True)
    second = jnp.mean(grad_hat * hat, axis=0, keepdims=True)
    return scale * (grad_hat - first - hat * second)


def rows_sum(value):
    ones = jnp.ones((8, value.shape[1]), jnp.bfloat16)
    total = 0.0
    for part in pair(value):
        total = total + lax.dot_general(ones, part, (NT, ((), ())), preferred_element_type=jnp.float32)
    return total


def spread_over(weights, masks, meshes):
    return jnp.concatenate([weights * masks[m : m + 1] for m in range(meshes)], axis=0)


def gathered_from(grad, masks, meshes):
    total = grad[:S] * masks[:1]
    for m in range(1, meshes):
        total = total + grad[m * S : (m + 1) * S] * masks[m : m + 1]
    return total


def both(reference, *at):
    return reference[(0,) + at], reference[(1,) + at]


def weights_of(routed, slice_t, cols, inverse, h):
    logits = (dot3(slice_t, pair(routed[h * DH : (h + 1) * DH])) + cols[:S, 9:10]) * inverse[h]
    top = jnp.max(logits, axis=0, keepdims=True)
    raised = jnp.exp(logits - top)
    return logits, raised / jnp.sum(raised, axis=0, keepdims=True)


def add_to(reference, value, at=...):
    @pl.when(pl.program_id(0) == 0)
    def _():
        reference[at] = value

    @pl.when(pl.program_id(0) > 0)
    def _():
        reference[at] = reference[at] + value


def slice_fwd(meshes, embeds, inv_ref, hid_ref, emb_ref, mask_ref, mt_ref, cols_ref, st_ref, *outs):
    if embeds:
        hidden_ref, feat_ref, rout_ref, w_ref, sums_ref = outs
        hidden = dot3(pair(emb_ref[:, :IN]), pair(hid_ref[...])) + emb_ref[:, IN : IN + 1]
        hidden_ref[...] = hidden
    else:
        feat_ref, rout_ref, w_ref, sums_ref = outs
        hidden = hid_ref[...]
    cols = cols_ref[...]
    masks = mask_ref[...]
    hat, _ = normed_of(hidden)
    normed = pair(hat * cols[:, 0:1] + cols[:, 1:2])
    features = dot3(both(mt_ref, 0), normed) + cols[:, 2:3]
    routed = dot3(both(mt_ref, 1), normed) + cols[:, 3:4]
    feat_ref[...] = features
    rout_ref[...] = routed
    slice_t = both(st_ref)
    ones = jnp.ones((8, hidden.shape[1]), jnp.float32)
    for h in range(H):
        _, weights = weights_of(routed, slice_t, cols, inv_ref, h)
        w_ref[h * S : (h + 1) * S] = weights
        wide = spread_over(weights, masks, meshes)
        tall = jnp.concatenate([features[h * DH : (h + 1) * DH], ones], axis=0)
        add_to(sums_ref, dot3(pair(tall), pair(wide), NT), h)


def out_fwd(meshes, heads_up, hid_ref, w_ref, mask_ref, mix_ref, mt_ref, cols_ref, *rest):
    if heads_up:
        tgt_ref, hd_ref, next_ref, mid_ref, pre_ref, spr_ref, err_ref = rest
    else:
        next_ref, mid_ref, pre_ref, spr_ref = rest
    cols = cols_ref[...]
    masks = mask_ref[...]
    parts = []
    for h in range(H):
        wide = spread_over(w_ref[h * S : (h + 1) * S], masks, meshes)
        parts.append(dot3(pair(mix_ref[h]), pair(wide)))
    spread = jnp.concatenate(parts, axis=0)
    spr_ref[...] = spread
    middle = hid_ref[...] + dot3(both(mt_ref, 2), pair(spread)) + cols[:, 4:5]
    mid_ref[...] = middle
    hat, _ = normed_of(middle)
    before = dot3(both(mt_ref, 3), pair(hat * cols[:, 5:6] + cols[:, 6:7])) + cols[:, 7:8]
    pre_ref[...] = before
    inner = 0.5 * before * (1.0 + lax.erf(before * 0.5**0.5))
    after = middle + dot3(both(mt_ref, 4), pair(inner)) + cols[:, 8:9]
    next_ref[...] = after
    if heads_up:
        hat, _ = normed_of(after)
        head = hd_ref[...]
        normed = hat * head[:, 8:9] + head[:, 9:10]
        misfit = dot3(pair(head[:, :8]), pair(normed), TN) + head[:8, 10:11] - tgt_ref[...]
        target = tgt_ref[...]
        error = jnp.sum(misfit * misfit, axis=0, keepdims=True)
        scale = jnp.sum(target * target, axis=0, keepdims=True)
        row = lax.broadcasted_iota(jnp.int32, (8, 1), 0)
        shaped = masks * jnp.where(row < meshes, error, 0.0)
        shaped_s = masks * scale
        both_sums = jnp.concatenate([shaped, shaped_s], axis=0)
        sums = jnp.broadcast_to(jnp.sum(both_sums, axis=1, keepdims=True), (16, 128))
        add_to(err_ref, sums)


def out_bwd(
    meshes, heads_up, grad_ref, mid_ref, pre_ref, spr_ref, w_ref, mask_ref, mix_ref, m_ref, cols_ref, *rest
):
    if heads_up:
        tgt_ref, hd_ref, scale_ref = rest[:3]
        rest = rest[3:]
    dmid_ref, dw_ref, dmix_ref, dm_ref, rows_ref = rest[:5]
    cols = cols_ref[...]
    masks = mask_ref[...]
    if heads_up:
        dhead_ref = rest[5]
        after = grad_ref[...]
        hat, scale = normed_of(after)
        head = hd_ref[...]
        normed = hat * head[:, 8:9] + head[:, 9:10]
        misfit = dot3(pair(head[:, :8]), pair(normed), TN) + head[:8, 10:11] - tgt_ref[...]
        per_point = jnp.sum(masks * scale_ref[:, :1], axis=0, keepdims=True)
        field = lax.broadcasted_iota(jnp.int32, (8, 1), 0)
        dpred = jnp.where(field < OUT, 2.0 * misfit * per_point, 0.0)
        dpred_pair = pair(dpred)
        dnormed = dot3(pair(head[:, :8]), dpred_pair)
        add_to(dhead_ref, dot3(dpred_pair, pair(normed), NT), 0)
        add_to(dhead_ref, jnp.broadcast_to(jnp.sum(dpred, axis=1, keepdims=True), (8, 256)), 1)
        add_to(dhead_ref, rows_sum(dnormed * hat), 2)
        add_to(dhead_ref, rows_sum(dnormed), 3)
        dafter = norm_back(dnormed * head[:, 8:9], hat, scale)
    else:
        dafter = grad_ref[...]
    before = pre_ref[...]
    cdf = 0.5 * (1.0 + lax.erf(before * 0.5**0.5))
    inner = before * cdf
    dafter_pair = pair(dafter)
    add_to(dm_ref, dot3(pair(inner), dafter_pair, NT), 2)
    add_to(rows_ref, rows_sum(dafter), 4)
    dinner = dot3(both(m_ref, 4), dafter_pair)
    slope = cdf + before * jnp.exp(-0.5 * before * before) * (1.0 / math.sqrt(2.0 * math.pi))
    dbefore = dinner * slope
    middle = mid_ref[...]
    hat, scale = normed_of(middle)
    normed = hat * cols[:, 5:6] + cols[:, 6:7]
    dbefore_pair = pair(dbefore)
    add_to(dm_ref, dot3(pair(normed), dbefore_pair, NT), 1)
    add_to(rows_ref, rows_sum(dbefore), 3)
    dnormed = dot3(both(m_ref, 3), dbefore_pair)
    add_to(rows_ref, rows_sum(dnormed * hat), 1)
    add_to(rows_ref, rows_sum(dnormed), 2)
    dmiddle = dafter + norm_back(dnormed * cols[:, 5:6], hat, scale)
    dmid_ref[...] = dmiddle
    dmiddle_pair = pair(dmiddle)
    add_to(dm_ref, dot3(pair(spr_ref[...]), dmiddle_pair, NT), 0)
    add_to(rows_ref, rows_sum(dmiddle), 0)
    dspread = dot3(both(m_ref, 2), dmiddle_pair)
    for h in range(H):
        wide = spread_over(w_ref[h * S : (h + 1) * S], masks, meshes)
        part = pair(dspread[h * DH : (h + 1) * DH])
        add_to(dmix_ref, dot3(part, pair(wide), NT), h)
        dwide = dot3(pair(mix_ref[h]), part, TN)
        dw_ref[h * S : (h + 1) * S] = gathered_from(dwide, masks, meshes)


def slice_bwd(
    meshes, embeds, inv_ref, hid_ref, feat_ref, rout_ref, w_ref, mask_ref, dsum_ref, dw_ref, dmid_ref, m_ref,
    cols_ref, st_ref, s_ref, *rest
):
    if embeds:
        in_ref, dm_ref, rows_ref, dsl_ref, dtemp_ref, demb_ref = rest
    else:
        dhid_ref, dm_ref, rows_ref, dsl_ref, dtemp_ref = rest
    cols = cols_ref[...]
    masks = mask_ref[...]
    slice_t, slice_w = both(st_ref), both(s_ref)
    routed = rout_ref[...]
    ones = jnp.ones((8, routed.shape[1]), jnp.float32)
    dfeat, drout = [], []
    for h in range(H):
        span = slice(h * DH, (h + 1) * DH)
        logits, weights = weights_of(routed, slice_t, cols, inv_ref, h)
        wide = spread_over(weights, masks, meshes)
        tall = jnp.concatenate([feat_ref[span], ones], axis=0)
        dsum = pair(dsum_ref[h])
        dwide = dot3(dsum, pair(tall), TN)
        dweights = gathered_from(dwide, masks, meshes) + dw_ref[h * S : (h + 1) * S]
        dtall = dot3(dsum, pair(wide))
        dfeat.append(dtall[:DH])
        dlogits = weights * (dweights - jnp.sum(weights * dweights, axis=0, keepdims=True))
        inner = dlogits * inv_ref[h]
        dtemp = jnp.sum(jnp.sum(inner * logits, axis=1, keepdims=True), axis=0, keepdims=True)
        add_to(dtemp_ref, jnp.broadcast_to(-dtemp, (8, 128)), h)
        inner_pair = pair(inner)
        drout.append(dot3(slice_w, inner_pair))
        lifted = jnp.concatenate([routed[span], ones], axis=0)
        add_to(dsl_ref, dot3(pair(lifted), inner_pair, NT), h)
    dfeatures = jnp.concatenate(dfeat, axis=0)
    drouted = jnp.concatenate(drout, axis=0)
    hidden = hid_ref[...]
    hat, scale = normed_of(hidden)
    normed = pair(hat * cols[:, 0:1] + cols[:, 1:2])
    dfeatures_pair, drouted_pair = pair(dfeatures), pair(drouted)
    add_to(dm_ref, dot3(normed, dfeatures_pair, NT), 0)
    add_to(dm_ref, dot3(normed, drouted_pair, NT), 1)
    add_to(rows_ref, rows_sum(dfeatures), 2)
    add_to(rows_ref, rows_sum(drouted), 3)
    dnormed = dot3(both(m_ref, 0), dfeatures_pair) + dot3(both(m_ref, 1), drouted_pair)
    add_to(rows_ref, rows_sum(dnormed * hat), 0)
    add_to(rows_ref, rows_sum(dnormed), 1)
    dhidden = dmid_ref[...] + norm_back(dnormed * cols[:, 0:1], hat, scale)
    if embeds:
        lifted = jnp.concatenate([in_ref[...], ones], axis=0)
        add_to(demb_ref, dot3(pair(lifted), pair(dhidden), NT))
    else:
        dhid_ref[...] = dhidden


def tile_call(kernel, name, inputs, outputs):
    points = next(a.shape[1] for kind, a in inputs if kind == "t")
    tile = min(TILE, points)

    def spec(kind, shape):
        if kind == "s":
            return pl.BlockSpec(memory_space=pltpu.SMEM)
        if kind == "t":
            return pl.BlockSpec((shape[0], tile), lambda i: (0, i))
        rank = len(shape)
        return pl.BlockSpec(tuple(shape), lambda i: (0,) * rank)

    return pl.pallas_call(
        kernel,
        grid=(points // tile,),
        in_specs=[spec(kind, a.shape) for kind, a in inputs],
        out_specs=[spec(kind, shape) for kind, shape in outputs],
        out_shape=[jax.ShapeDtypeStruct(shape, jnp.float32) for _, shape in outputs],
        compiler_params=pltpu.CompilerParams(
            dimension_semantics=("arbitrary",), vmem_limit_bytes=VMEM_CAP
        ),
        name=name,
    )(*[a for _, a in inputs])


def mix_head(sums, triple, meshes):
    tokens = sums[:DH] / (sums[DH : DH + 1] + 1e-05)
    tokens_pair = pair(tokens)
    queries = dot3(both(triple, 0), tokens_pair)
    keys_all = dot3(both(triple, 1), tokens_pair)
    values = dot3(both(triple, 2), tokens_pair)
    scores = dot3(pair(keys_all), pair(queries), TN) * DH ** (-0.5)
    wide = meshes * S
    group_t = lax.broadcasted_iota(jnp.int32, (wide, wide), 0) // S
    group_s = lax.broadcasted_iota(jnp.int32, (wide, wide), 1) // S
    inside = group_t == group_s
    top = jnp.max(jnp.where(inside, scores, -3.0e38), axis=0, keepdims=True)
    raised = jnp.where(inside, jnp.exp(jnp.where(inside, scores - top, 0.0)), 0.0)
    probs = raised / jnp.sum(raised, axis=0, keepdims=True)
    return tokens, queries, keys_all, values, probs


def mix_fwd(meshes, own, own_ref, triple_ref, out_ref):
    for h in range(own):
        _, _, _, values, probs = mix_head(own_ref[h], triple_ref, meshes)
        out_ref[h] = dot3(pair(values), pair(probs))


def mix_bwd(meshes, own, own_ref, dmix_ref, triple_ref, plain_ref, out_ref, dtriple_ref):
    for h in range(own):
        sums = own_ref[h]
        tokens, queries, keys_all, values, probs = mix_head(sums, triple_ref, meshes)
        dmix = dmix_ref[h]
        dmix_pair, probs_pair = pair(dmix), pair(probs)
        dvalues = dot3(dmix_pair, probs_pair, NT)
        dprobs = dot3(pair(values), dmix_pair, TN)
        dscores = probs * (dprobs - jnp.sum(probs * dprobs, axis=0, keepdims=True)) * DH ** (-0.5)
        dscores_pair = pair(dscores)
        dqueries = dot3(pair(keys_all), dscores_pair)
        dkeys = dot3(pair(queries), dscores_pair, NT)
        tokens_pair = pair(tokens)
        dtokens = 0.0
        for index, grad in enumerate((dqueries, dkeys, dvalues)):
            grad_pair = pair(grad)
            dtokens = dtokens + dot3(both(plain_ref, index), grad_pair)
            weight = dot3(tokens_pair, grad_pair, NT)
            if h == 0:
                dtriple_ref[index] = weight
            else:
                dtriple_ref[index] = dtriple_ref[index] + weight
        under = 1.0 / (sums[DH : DH + 1] + 1e-05)
        dnum = dtokens * under
        dden = -jnp.sum(dnum * tokens, axis=0, keepdims=True)
        out_ref[h] = jnp.concatenate([dnum, dden, jnp.zeros((7, meshes * S), jnp.float32)], axis=0)


def pts_greet(size, place):
    barrier = pltpu.get_barrier_semaphore()
    for step in range(1, size):
        pl.semaphore_signal(
            barrier, inc=1, device_id={"pts": lax.rem(place + step, size)}, device_id_type=MESH
        )
    pl.semaphore_wait(barrier, size - 1)


def reduce_heads(size, place, part, landing, total, mail):
    own = part.shape[0] // size
    waits = []
    for step in range(1, size):
        other = lax.rem(place + step, size)
        waits.append(mail.send(part.at[pl.ds(other * own, own)], landing.at[step - 1], {"pts": other}))
    for copy in waits:
        copy.wait_recv()
    value = part[pl.ds(place * own, own)]
    for step in range(size - 1):
        value = value + landing[step]
    total[...] = value


def share_heads(size, place, piece, full, mail):
    own = piece.shape[0]
    full[pl.ds(place * own, own)] = piece[...]
    waits = []
    for step in range(1, size):
        other = lax.rem(place + step, size)
        waits.append(mail.send(piece, full.at[pl.ds(place * own, own)], {"pts": other}))
    for copy in waits:
        copy.wait_recv()


def mix_fwd_kernel(size, meshes, part, triple, out, total, landing, piece, send_sems, recv_sems):
    place = lax.axis_index("pts")
    pts_greet(size, place)
    mail = Mail(send_sems, recv_sems)
    reduce_heads(size, place, part, landing, total, mail)
    mix_fwd(meshes, total.shape[0], total, triple, piece)
    share_heads(size, place, piece, out, mail)
    mail.close()


def mix_bwd_kernel(size, meshes, part, sums, triple, plain, out, dtriple, total, landing, piece, send_sems, recv_sems):
    place = lax.axis_index("pts")
    pts_greet(size, place)
    mail = Mail(send_sems, recv_sems)
    reduce_heads(size, place, part, landing, total, mail)
    mix_bwd(meshes, total.shape[0], sums, total, triple, plain, piece, dtriple)
    share_heads(size, place, piece, out, mail)
    mail.close()


def loss_kernel(size, meshes, total_meshes, floor_value, sums, scale_out, loss_out, total, send_sems, recv_sems):
    place = lax.axis_index("pts")
    pts_greet(size, place)
    mail = Mail(send_sems, recv_sems)
    total[place] = sums[...]
    waits = []
    for step in range(1, size):
        waits.append(mail.send(sums, total.at[place], {"pts": lax.rem(place + step, size)}))
    for copy in waits:
        copy.wait_recv()
    value = total[0]
    for index in range(1, size):
        value = value + total[index]
    errors, scales = value[:8] + 1e-06, jnp.maximum(value[8:], floor_value)
    root = jnp.sqrt(errors / scales)
    row = lax.broadcasted_iota(jnp.int32, (8, 128), 0)
    scale_out[...] = jnp.where(row < meshes, 0.5 / (root * scales * total_meshes), 0.0)
    terms = jnp.where(row < meshes, root, 0.0)
    loss_out[...] = jnp.broadcast_to(
        jnp.sum(terms, axis=0, keepdims=True) / total_meshes, (8, 128)
    )
    mail.close()


def comm_call(kernel, name, number, inputs, outputs, scratch, copies):
    vmem = pl.BlockSpec(memory_space=pltpu.VMEM)
    dma = pltpu.SemaphoreType.DMA
    return pl.pallas_call(
        kernel,
        in_specs=[vmem] * len(inputs),
        out_specs=[vmem] * len(outputs),
        out_shape=[jax.ShapeDtypeStruct(shape, jnp.float32) for shape in outputs],
        scratch_shapes=[pltpu.VMEM(shape, jnp.float32) for shape in scratch]
        + [dma((copies,)), dma((copies,))],
        compiler_params=pltpu.CompilerParams(
            collective_id=number, has_side_effects=True, vmem_limit_bytes=VMEM_CAP
        ),
        name=name,
    )(*inputs)


def local(
    inputs,
    target,
    lengths,
    step_count,
    muon_weight,
    muon_moment,
    adam_weight,
    adam_first,
    adam_second,
):
    muon_all, adam_all = (
        lax.all_gather(muon_weight, ("mesh", "pts"), axis=2, tiled=True),
        lax.all_gather(adam_weight, ("mesh", "pts"), axis=0, tiled=True),
    )
    points = inputs.shape[0]
    pts_count = lax.axis_size("pts")
    floor_value = float(points * pts_count)
    onehot = mesh_mask(lengths[0], lax.axis_index("pts") * points, points)
    meshes = lax.axis_size("mesh") * lengths.shape[1]
    hidden, embed_back = jax.vjp(lambda packed: embed_piece(inputs, packed), adam_all)
    saved = []
    for layer_index in range(L):
        matrices = muon_all[layer_index]
        (weights, numerator, denominator), slice_back = jax.vjp(
            partial(slice_piece, layer_index=layer_index, onehot=onehot), hidden, matrices, adam_all
        )
        numerator, denominator = lax.psum((numerator, denominator), "pts")
        mixed, mix_back = jax.vjp(
            partial(mix_piece, layer_index=layer_index), numerator, denominator, adam_all
        )
        following, out_back = jax.vjp(
            partial(out_piece, layer_index=layer_index, onehot=onehot),
            hidden,
            weights,
            mixed,
            matrices,
            adam_all,
        )
        saved.append((slice_back, mix_back, out_back))
        hidden = following
    (errors, scales), head_back = jax.vjp(
        lambda state, packed: head_piece(state, packed, target, onehot), hidden, adam_all
    )
    errors, scales = lax.psum((errors, scales), "pts")
    group_loss, loss_back = jax.vjp(
        lambda first, second: loss_piece(first, second, meshes, floor_value), errors, scales
    )
    grad_errors, grad_scales = loss_back(jnp.ones_like(group_loss))
    grad_hidden, grad_adam = head_back((grad_errors, grad_scales))
    grad_layers = [None] * L
    for layer_index in reversed(range(L)):
        slice_back, mix_back, out_back = saved[layer_index]
        grad_hidden_out, grad_weights, grad_mixed, grad_mats_out, grad_adam_out = out_back(
            grad_hidden
        )
        grad_mixed = lax.psum(grad_mixed, "pts")
        grad_num, grad_den, grad_adam_mix = mix_back(grad_mixed)
        grad_hidden_in, grad_mats_in, grad_adam_in = slice_back((grad_weights, grad_num, grad_den))
        grad_hidden = grad_hidden_out + grad_hidden_in
        grad_adam = grad_adam + grad_adam_out + grad_adam_in + grad_adam_mix / pts_count
        grad_layers[layer_index] = grad_mats_out + grad_mats_in
    (grad_embed,) = embed_back(grad_hidden)
    grad_adam = grad_adam + grad_embed
    grad_muon = jnp.stack(grad_layers)
    grad_muon, grad_adam = (
        lax.psum_scatter(grad_muon, ("mesh", "pts"), scatter_dimension=2, tiled=True),
        lax.psum_scatter(grad_adam, ("mesh", "pts"), scatter_dimension=0, tiled=True),
    )
    square_sum, loss_total = lax.psum(
        (jnp.sum(grad_muon * grad_muon) + jnp.sum(grad_adam * grad_adam), group_loss / pts_count),
        ("mesh", "pts"),
    )

    def frob_of(moment):
        return lax.psum(jnp.sum(moment * moment, axis=(2, 3)), ("mesh", "pts"))

    def orthogonal_of(normalized):
        groups = lax.axis_size("mesh")
        count_all = normalized.shape[0] * normalized.shape[1]
        per_group = (count_all + groups - 1) // groups
        stacked = normalized.reshape((count_all,) + normalized.shape[2:])
        filler = jnp.zeros((per_group * groups - count_all,) + normalized.shape[2:], jnp.float32)
        spread = lax.all_to_all(
            jnp.concatenate([stacked, filler], axis=0),
            "mesh",
            split_axis=0,
            concat_axis=1,
            tiled=True,
        )

        def gram_of(current):
            return lax.psum(jnp.einsum("krc,krd->kcd", current, current, precision=HIGH), "pts")

        finished = newton_schulz(spread, gram_of)
        returned = lax.all_to_all(finished, "mesh", split_axis=1, concat_axis=0, tiled=True)
        return returned[:count_all].reshape(normalized.shape)

    results = apply_update(
        grad_muon,
        grad_adam,
        square_sum,
        step_count,
        muon_weight,
        muon_moment,
        adam_weight,
        adam_first,
        adam_second,
        frob_of,
        orthogonal_of,
    )
    return (results[0], results[1], results[2], results[3], results[4], loss_total, results[5])


def local_fast(
    inputs,
    target,
    lengths,
    step_count,
    muon_weight,
    muon_moment,
    adam_weight,
    adam_first,
    adam_second,
):
    mesh_count, pts_count = lax.axis_size("mesh"), lax.axis_size("pts")
    dims = grid_of(mesh_count, pts_count)
    planes, rows, columns, cores = dims
    count = mesh_count * pts_count
    shard, span = adam_weight.shape[0], muon_weight.shape[2]
    mats = muon_weight.shape[0] * muon_weight.shape[1]
    slabs = span // 8
    pad = -(-shard // 2048) * 2048

    def slab_of(vector):
        return jnp.pad(vector, (0, pad - shard)).reshape(-1, 8, 256)

    def stacked(value):
        return value.reshape(mats * slabs, 8, 256)

    half = muon_weight.shape[1] * slabs
    all_first, all_second, all_vector = gather_all(
        dims, muon_weight[0].reshape(half, 8, 256), muon_weight[1].reshape(half, 8, 256), slab_of(adam_weight)
    )

    def matrices_of(value, order):
        value = value.reshape(value.shape[:4] + (half // slabs, slabs, 8, 256))
        value = jnp.transpose(value, (4,) + order + (5, 6, 7))
        return value.reshape(half // slabs, count * span, 256)

    muon_all = (
        matrices_of(all_first, (3, 2, 1, 0)), matrices_of(all_second, (3, 1, 2, 0))
    )
    adam_all = jnp.transpose(all_vector, (3, 2, 1, 0, 4, 5, 6)).reshape(count, pad)[:, :shard].reshape(-1)
    points = inputs.shape[0]
    floor_value = float(points * pts_count)
    meshes = lengths.shape[1]
    params = unpack(adam_all)
    masks = mesh_mask(lengths[0], lax.axis_index("pts") * points, points).T
    masks = jnp.pad(masks, ((0, 8 - meshes), (0, 0)))
    inputs_t = inputs.T
    target_t = jnp.pad(target.T, ((0, 8 - OUT), (0, 0)))

    def halves(value):
        high = lax.reduce_precision(value, 8, 7)
        return jnp.stack([high, value - high]).astype(jnp.bfloat16)

    def columns_of(*values):
        tall = [jnp.pad(v, ((0, C - v.shape[0]), (0, 0))) for v in values]
        wide = sum(v.shape[1] for v in tall)
        return jnp.pad(jnp.concatenate(tall, axis=1), ((0, 0), (0, 16 - wide)))

    embed = columns_of(params["emb_w"].T, params["emb_b"][:, None])
    head = columns_of(
        jnp.pad(params["head_w"], ((0, 0), (0, 8 - OUT))), params["fin"].T, params["head_b"][:, None]
    )
    plain = [halves(muon_all[l]) for l in range(L)]
    turned = [jnp.swapaxes(plain[l], 2, 3) for l in range(L)]
    cols = [columns_of(params["vec"][l].T, params["slice_b"][l][:, None]) for l in range(L)]
    slice_w = [halves(params["slice_w"][l]) for l in range(L)]
    slice_t = [jnp.swapaxes(slice_w[l], 1, 2) for l in range(L)]
    triple = [halves(params["qkv"][l]) for l in range(L)]
    triple_t = [jnp.swapaxes(triple[l], 2, 3) for l in range(L)]
    inverse = [1.0 / params["temp"][l] for l in range(L)]
    own = H // pts_count
    wide = meshes * S
    kept = []
    hidden = inputs_t
    for l in range(L):
        embeds, heads_up = l == 0, l == L - 1
        outs = [("t", (C, points))] if embeds else []
        outs += [("t", (C, points))] * 2 + [("t", (H * S, points)), ("w", (H, DH + 8, wide))]
        found = tile_call(
            partial(slice_fwd, meshes, embeds), "slice_fwd",
            [("s", inverse[l]), ("t", hidden), ("w", embed), ("t", masks), ("w", turned[l]), ("w", cols[l]), ("w", slice_t[l])],
            outs,
        )
        if embeds:
            hidden = found[0]
        features, routed, weights, sums = found[-4:]
        mixed, own_sums = comm_call(
            partial(mix_fwd_kernel, pts_count, meshes), "mix_fwd", 2 + l,
            [sums, triple_t[l]],
            [(H, DH, wide), (own, DH + 8, wide)],
            [(max(pts_count - 1, 1), own, DH + 8, wide), (own, DH, wide)],
            2 * pts_count,
        )
        given = [("t", hidden), ("t", weights), ("t", masks), ("w", mixed), ("w", turned[l]), ("w", cols[l])]
        outs = [("t", (C, points))] * 4
        if heads_up:
            given += [("t", target_t), ("w", head)]
            outs += [("w", (16, 128))]
        found = tile_call(partial(out_fwd, meshes, heads_up), "out_fwd", given, outs)
        kept.append((hidden, features, routed, weights, own_sums, mixed) + tuple(found[1:4]))
        hidden = found[0]
    total_meshes = float(mesh_count * meshes)
    scale, loss = comm_call(
        partial(loss_kernel, pts_count, meshes, total_meshes, floor_value), "loss_sums", 2 + 2 * L,
        [found[4]],
        [(8, 128), (8, 128)],
        [(pts_count, 16, 128)],
        pts_count,
    )
    group_loss = loss[0, 0]
    grad = hidden
    grad_layers, vec_rows, slices, temps, triples = [None] * L, [None] * L, [None] * L, [None] * L, [None] * L
    for l in reversed(range(L)):
        embeds, heads_up = l == 0, l == L - 1
        hidden, features, routed, weights, own_sums, mixed, middle, before, spread = kept[l]
        given = [
            ("t", grad), ("t", middle), ("t", before), ("t", spread), ("t", weights), ("t", masks), ("w", mixed),
            ("w", plain[l]), ("w", cols[l]),
        ]
        outs = [
            ("t", (C, points)), ("t", (H * S, points)), ("w", (H, DH, wide)), ("w", (3, C, C)), ("w", (5, 8, C)),
        ]
        if heads_up:
            given += [("t", target_t), ("w", head), ("w", scale)]
            outs += [("w", (4, 8, C))]
        found = tile_call(partial(out_bwd, meshes, heads_up), "out_bwd", given, outs)
        dmiddle, dweights, dmixed, dmats_out, rows_out = found[:5]
        if heads_up:
            dhead = found[5]
        dsums, triples[l] = comm_call(
            partial(mix_bwd_kernel, pts_count, meshes), "mix_bwd", 3 + 2 * L + l,
            [dmixed, own_sums, triple_t[l], triple[l]],
            [(H, DH + 8, wide), (3, DH, DH)],
            [(own, DH, wide), (max(pts_count - 1, 1), own, DH, wide), (own, DH + 8, wide)],
            2 * pts_count,
        )
        given = [
            ("s", inverse[l]), ("t", hidden), ("t", features), ("t", routed), ("t", weights), ("t", masks), ("w", dsums),
            ("t", dweights), ("t", dmiddle), ("w", plain[l]), ("w", cols[l]), ("w", slice_t[l]), ("w", slice_w[l]),
        ]
        outs = [("w", (2, C, C)), ("w", (4, 8, C)), ("w", (H, DH + 8, S)), ("w", (H, 8, 128))]
        if embeds:
            given += [("t", inputs_t)]
            outs += [("w", (16, C))]
        else:
            outs = [("t", (C, points))] + outs
        found = tile_call(partial(slice_bwd, meshes, embeds), "slice_bwd", given, outs)
        if embeds:
            dembed = found[-1]
            found = found[:-1]
        else:
            grad = found[0]
            found = found[1:]
        dmats_in, rows_in, slices[l], temps[l] = found
        slices[l] = jnp.sum(slices[l], axis=0)
        temps[l] = temps[l][:, 0, 0]
        grad_layers[l] = jnp.concatenate([dmats_in, dmats_out], axis=0)
        vec_rows[l] = jnp.concatenate([rows_in[:, 0], rows_out[:, 0]], axis=0)
    pieces = [
        dembed[: IN + 1].reshape(-1),
        dhead[0, :OUT].T.reshape(-1),
        dhead[1, :OUT, 0],
        dhead[2:, 0].reshape(-1),
        jnp.stack(triples).reshape(-1),
        jnp.stack([s[:DH] for s in slices]).reshape(-1),
        jnp.stack([s[DH] for s in slices]).reshape(-1),
        jnp.stack(temps).reshape(-1),
        jnp.stack(vec_rows).reshape(-1),
    ]
    grad_adam = jnp.concatenate(pieces)
    grad_adam = jnp.pad(grad_adam, (0, adam_all.shape[0] - grad_adam.shape[0]))
    def parts_of(value, order):
        value = value.reshape(half // slabs, planes, rows, columns, cores, slabs, 8, 256)
        value = jnp.transpose(value, order + (0, 5, 6, 7))
        return value.reshape(value.shape[:4] + (half, 8, 256))

    adam_parts = jnp.pad(grad_adam.reshape(count, shard), ((0, 0), (0, pad - shard)))
    adam_parts = adam_parts.reshape(planes, rows, columns, cores, -1, 8, 256)
    adam_parts = jnp.transpose(adam_parts, (3, 2, 1, 0, 4, 5, 6))
    step = step_count[0].astype(jnp.float32)
    rates = jnp.stack([one_cycle(step), 1.0 - 0.9**step, 1.0 - 0.999**step])
    results = tail_update(
        dims,
        parts_of(grad_layers[0], (4, 3, 2, 1)),
        parts_of(grad_layers[1], (4, 2, 3, 1)),
        adam_parts,
        jnp.reshape(group_loss / pts_count, (1,)),
        rates,
        stacked(muon_weight),
        stacked(muon_moment),
        slab_of(adam_weight),
        slab_of(adam_first),
        slab_of(adam_second),
    )

    def unslab(value):
        return value.reshape(-1)[:shard]

    return (
        results[0].reshape(muon_weight.shape),
        results[1].reshape(muon_weight.shape),
        unslab(results[2]),
        unslab(results[3]),
        unslab(results[4]),
        results[5][1, 0],
        results[5][0, 0],
    )


def solution(mesh):
    in_specs = (
        P(("mesh", "pts"), None),
        P(("mesh", "pts"), None),
        P("mesh", None),
        P(),
        P(None, None, ("mesh", "pts"), None),
        P(None, None, ("mesh", "pts"), None),
        P(("mesh", "pts")),
        P(("mesh", "pts")),
        P(("mesh", "pts")),
    )
    out_specs = (
        P(None, None, ("mesh", "pts"), None),
        P(None, None, ("mesh", "pts"), None),
        P(("mesh", "pts")),
        P(("mesh", "pts")),
        P(("mesh", "pts")),
        P(),
        P(),
    )
    def chosen(*args):
        return (local_fast if args[4].shape[2] == 8 else local)(*args)

    return jax.shard_map(chosen, mesh=mesh, in_specs=in_specs, out_specs=out_specs, check_vma=False)
```
